32 devices in a mesh: dom: 32 (over z, y, x, core).
Axes of the slice: x: 2, y: 2, z: 4, core: 2. Of those that a mesh axis runs over, the one named last changes fastest.
Arguments:
- features: bfloat16 [8192, 512], P('dom'), may hold values from -6 to 6
- w_one: bfloat16 [9, 512, 512], replicated, may hold values from -0.25 to 0.25
- w_two: bfloat16 [8, 512, 349], replicated, may hold values from -0.25 to 0.25
- self_two: bfloat16 [512, 349], replicated, may hold values from -80 to 80
- edge_src: int32 [8, 64, 256], P(None, 'dom'), may hold values from 0 to 511, as said below
- edge_dst: int32 [8, 64, 256], P(None, 'dom'), may hold values from -1 to 127, as said below
- send_rows: int32 [32, 32, 8], P('dom'), may hold values from 0 to 255
- send_count: int32 [32, 32], P('dom'), may hold values from 1 to 8, as said below
- labels: int32 [8192], P('dom'), may hold values from -1 to 348
Outputs:
- logits: float32 [8192, 349], P('dom')
- loss: float32 [], replicated
- grad_one: float32 [4608, 512], P('dom')
- grad_two: float32 [4608, 349], P('dom')
The draws below stay inside these ranges and needn't reach their ends.
Inputs may be any that keep to these rules, and one draw needn't show every extreme that they name: `send_rows`: entry [p, q, s] is a row of partition p's own nodes, rows may repeat. `send_count`: entry [p, q] counts the live slots p sends to q; every row reaches 8 at some q. `edge_src`: index into the destination partition's table: its 256 own rows, then 8 slots from each partition in order. `edge_dst`: -1 marks an empty edge slot.
All inputs are finite; a program needn't handle non-finite values.
Results may differ from the reference program's by a relative error of at most 0.0085.
The reference program's roundings to bfloat16 on the way count: a program that leaves them out, or rounds other values in their place, can miss the bound.
Values may be sent and summed in bfloat16 or wider, within the bound.
No kernel may reach another device: no remote copies, remote signals or barrier semaphores. Data moves between devices by JAX's collectives and lax.ppermute only.
A program may use at most 128 MiB of HBM per device.

```python
import jax
import jax.numpy as jnp
from jax import lax

D = 512
CLASSES = 349
RELATIONS = 8
NODES_DEV = 256
SLOTS = 8
EDGES_BLOCK = 256
NODES = 8192
N_DOM = 32


def slot_counts(key):
    base_key = jax.random.fold_in(key, 7)
    limits = jax.random.randint(jax.random.fold_in(base_key, 1), (N_DOM, 1), 1, SLOTS + 1)
    counts = jax.random.randint(jax.random.fold_in(base_key, 2), (N_DOM, N_DOM), 1, SLOTS + 1)
    counts = jnp.minimum(counts, limits)
    full_peer = jax.random.randint(jax.random.fold_in(base_key, 3), (N_DOM, 1), 0, N_DOM)
    peer_ids = jnp.arange(N_DOM, dtype=jnp.int32)[None, :]
    return jnp.where(peer_ids == full_peer, SLOTS, counts).astype(jnp.int32)


def edge_tables(key):
    counts = slot_counts(key)
    base_key = jax.random.fold_in(key, 11)
    blocks = NODES // 128
    edge_shape = (RELATIONS, blocks, EDGES_BLOCK)
    owner_dev = (jnp.arange(blocks, dtype=jnp.int32) // (NODES_DEV // 128))[None, :, None] * jnp.ones(edge_shape, jnp.int32)
    live_level = jax.random.randint(jax.random.fold_in(base_key, 1), (N_DOM,), 4, 11)
    live_edge = jax.random.randint(jax.random.fold_in(base_key, 2), edge_shape, 0, 10) < live_level[owner_dev]
    targets = jnp.where(live_edge, jax.random.randint(jax.random.fold_in(base_key, 3), edge_shape, 0, 128), -1)
    remote = jax.random.randint(jax.random.fold_in(base_key, 4), edge_shape, 0, 2) == 1
    peer_pick = jax.random.randint(jax.random.fold_in(base_key, 5), edge_shape, 0, N_DOM)
    slot_limit = counts[peer_pick, owner_dev]
    slot_pick = jax.random.randint(jax.random.fold_in(base_key, 6), edge_shape, 0, 1 << 20) % slot_limit
    remote_row = NODES_DEV + peer_pick * SLOTS + slot_pick
    local_row = jax.random.randint(jax.random.fold_in(base_key, 7), edge_shape, 0, NODES_DEV)
    sources = jnp.where(remote, remote_row, local_row)
    return (sources.astype(jnp.int32), targets.astype(jnp.int32))


def draw_send_count(key, part):
    return slot_counts(key)


def draw_edge_src(key, part):
    return edge_tables(key)[0]


def draw_edge_dst(key, part):
    return edge_tables(key)[1]


def draw_labels(key, part):
    base_key = jax.random.fold_in(key, 23)
    device_of = jnp.arange(NODES, dtype=jnp.int32) // NODES_DEV
    chance = jax.random.randint(jax.random.fold_in(base_key, 1), (NODES,), 0, 1000)
    labelled = chance < 250 + 500 * device_of // max(N_DOM - 1, 1)
    classes = jax.random.randint(jax.random.fold_in(base_key, 2), (NODES,), 0, CLASSES)
    return jnp.where(labelled, classes, -1).astype(jnp.int32)


def draw_self_two(key, part):
    base_key = jax.random.fold_in(key, 31)
    values = jax.random.normal(jax.random.fold_in(base_key, 1), (D, CLASSES), jnp.float32) * D ** (-0.5)
    return jnp.clip(values, -80.0, 80.0).astype(jnp.bfloat16)


def set_ends(drawn, own_key, least, top_value):
    spot = [jax.random.randint(jax.random.fold_in(own_key, axis), (), 0, length) for axis, length in enumerate(drawn.shape)]
    widest = drawn.shape.index(max(drawn.shape))
    neighbour = spot[:widest] + [(spot[widest] + 1) % drawn.shape[widest]] + spot[widest + 1:]
    return drawn.at[tuple(spot)].set(least).at[tuple(neighbour)].set(top_value)


def level_of(rng, shape, shards, least, high):
    def one(position, shards_of):
        heights = jax.random.uniform(jax.random.fold_in(jax.random.fold_in(rng, 6), position), (shards_of,), jnp.float32, least / len(shards), high / len(shards))
        return jnp.repeat(jnp.exp(heights), shape[position] // shards_of).reshape((-1,) + (1,) * (len(shape) - position - 1))

    level = one(*shards[0])
    for cut in shards[1:]:
        level = level * one(*cut)
    return level


def scatter_about(key, shape, scale, bound, cuts=(), kind=jnp.bfloat16):
    factor_of = level_of(key, shape, cuts, -0.22, 0.18) if cuts else 1.0
    array = jax.random.normal(key, shape, jnp.float32) * scale * factor_of
    return jnp.minimum(jnp.maximum(array, -bound), bound).astype(kind)


def setup_inputs(seed: int = 0) -> dict:
    keys = jax.random.split(jax.random.key(seed), 10)
    return {
        "features": scatter_about(keys[0], (NODES, D), 1.0, 6.0, ((0, 32),)),
        "w_one": scatter_about(keys[1], (RELATIONS + 1, D, D), D ** -0.5, 0.25),
        "w_two": scatter_about(keys[2], (RELATIONS, D, CLASSES), D ** -0.5, 0.25),
        "self_two": draw_self_two(jax.random.fold_in(keys[9], 71), 0),
        "edge_src": draw_edge_src(jax.random.fold_in(keys[9], 71), 0),
        "edge_dst": draw_edge_dst(jax.random.fold_in(keys[9], 71), 0),
        "send_rows": set_ends(jax.random.randint(keys[6], (N_DOM, N_DOM, SLOTS), 0, NODES_DEV), jax.random.fold_in(keys[6], 1), 0, NODES_DEV - 1).astype(jnp.int32),
        "send_count": draw_send_count(jax.random.fold_in(keys[9], 71), 0),
        "labels": draw_labels(jax.random.fold_in(keys[9], 71), 0),
    }


loss_scale = 256.0


def slot_rows(values, send_rows, send_count, device):
    picks = send_rows[:, device, :]
    owners = jnp.arange(N_DOM, dtype=jnp.int32)[:, None] * NODES_DEV + picks
    chosen = values[owners.reshape(-1)]
    live_slot = (jnp.arange(SLOTS, dtype=jnp.int32)[None, :] < send_count[:, device][:, None]).reshape(-1)
    return jnp.where(live_slot[:, None], chosen, jnp.zeros_like(chosen))


def device_edges(edge_src, edge_dst, device):
    blocks = NODES_DEV // 128
    start = (device * blocks).astype(jnp.int32)
    return (lax.dynamic_slice_in_dim(edge_src, start, blocks, 1), lax.dynamic_slice_in_dim(edge_dst, start, blocks, 1))


def edge_targets(targets):
    blocks = NODES_DEV // 128
    live_edge = targets >= 0
    node_of = jnp.arange(blocks, dtype=jnp.int32)[None, :, None] * 128 + jnp.where(live_edge, targets, 0)
    segment = jnp.arange(RELATIONS, dtype=jnp.int32)[:, None, None] * NODES_DEV + node_of
    return jnp.where(live_edge, segment, RELATIONS * NODES_DEV).reshape(-1).astype(jnp.int32)


def aggregate(node_table, sources, targets):
    segment = edge_targets(targets)
    slots_all = RELATIONS * NODES_DEV + 1
    gathered = node_table[sources.reshape(-1)].astype(jnp.float32)
    sums = jax.ops.segment_sum(gathered, segment, num_segments=slots_all)[:-1]
    counts = jax.ops.segment_sum(jnp.ones(segment.shape, jnp.float32), segment, num_segments=slots_all)[:-1]
    norm_rows = 1.0 / jnp.maximum(counts, 1.0)
    averaged = (sums * norm_rows[:, None]).astype(jnp.bfloat16)
    return averaged.reshape(RELATIONS, NODES_DEV, -1), norm_rows.reshape(RELATIONS, NODES_DEV)


def layer(device, values, weights, self_weight, send_rows, send_count, edge_src, edge_dst):
    own_rows = lax.dynamic_slice_in_dim(values, (device * NODES_DEV).astype(jnp.int32), NODES_DEV, 0)
    node_table = jnp.concatenate([own_rows, slot_rows(values, send_rows, send_count, device)], axis=0)
    sources, targets = device_edges(edge_src, edge_dst, device)
    averaged, norm_rows = aggregate(node_table, sources, targets)
    output = jnp.einsum('rnd,rde->ne', averaged.astype(jnp.float32), weights.astype(jnp.float32))
    output = output + jnp.dot(own_rows, self_weight, preferred_element_type=jnp.float32)
    return own_rows, averaged, norm_rows, sources, targets, output


def reference(features, w_one, w_two, self_two, edge_src, edge_dst, send_rows, send_count, labels):
    devices = jnp.arange(N_DOM, dtype=jnp.int32)

    def first(device):
        return layer(device, features, w_one[:RELATIONS], w_one[RELATIONS], send_rows, send_count, edge_src, edge_dst)

    def second(device, hidden):
        return layer(device, hidden, w_two, self_two, send_rows, send_count, edge_src, edge_dst)

    hidden = lax.map(lambda device: jnp.maximum(first(device)[5], 0.0).astype(jnp.bfloat16), devices).reshape(NODES, D)
    logits = lax.map(lambda device: second(device, hidden)[5], devices).reshape(NODES, CLASSES)

    labelled = labels >= 0
    log_total = jax.nn.logsumexp(logits, axis=1)
    one_hot = (jnp.arange(CLASSES, dtype=jnp.int32)[None, :] == labels[:, None]).astype(jnp.float32)
    picked = jnp.sum(logits * one_hot, axis=1)
    total = jnp.sum(jnp.where(labelled, log_total - picked, 0.0))
    label_count = jnp.sum(labelled.astype(jnp.float32))
    loss = total / label_count
    softmax_out = jnp.exp(logits - log_total[:, None])
    grad_logits = (loss_scale * (softmax_out - one_hot) * labelled[:, None].astype(jnp.float32) / label_count).astype(jnp.bfloat16)

    table_rows = NODES_DEV + N_DOM * SLOTS

    def back_two(carry, device):
        own_rows, averaged, norm_rows, sources, targets, unused = second(device, hidden)
        grad_rows = lax.dynamic_slice_in_dim(grad_logits, (device * NODES_DEV).astype(jnp.int32), NODES_DEV, 0)
        grad_term = jnp.concatenate([
            jnp.einsum('rnd,nc->rdc', averaged.astype(jnp.float32), grad_rows.astype(jnp.float32)),
            jnp.dot(own_rows.T, grad_rows, preferred_element_type=jnp.float32)[None]], axis=0)
        spread = (jnp.einsum('nc,rdc->rnd', grad_rows.astype(jnp.float32), w_two.astype(jnp.float32)) * norm_rows[:, :, None]).astype(jnp.bfloat16)
        segment = edge_targets(targets)
        padded = jnp.concatenate([spread.reshape(RELATIONS * NODES_DEV, D), jnp.zeros((1, D), jnp.bfloat16)], axis=0)
        per_edge = padded[segment].astype(jnp.float32)
        table_grad = jax.ops.segment_sum(per_edge, sources.reshape(-1), num_segments=table_rows)
        local_grad = table_grad[:NODES_DEV] + jnp.dot(grad_rows, self_two.T, preferred_element_type=jnp.float32)
        return carry + grad_term, (local_grad, table_grad[NODES_DEV:].astype(jnp.bfloat16))

    grad_two, outputs = lax.scan(back_two, jnp.zeros((RELATIONS + 1, D, CLASSES), jnp.float32), devices)
    local_grads, backs = outputs

    owners = jnp.arange(N_DOM, dtype=jnp.int32)[None, :, None] * NODES_DEV + jnp.swapaxes(send_rows, 0, 1)
    live_slot = jnp.arange(SLOTS, dtype=jnp.int32)[None, None, :] < jnp.swapaxes(send_count, 0, 1)[:, :, None]
    back_values = jnp.where(live_slot[..., None], backs.reshape(N_DOM, N_DOM, SLOTS, D).astype(jnp.float32), 0.0)
    returned = jax.ops.segment_sum(back_values.reshape(-1, D), owners.reshape(-1), num_segments=NODES)
    grad_hidden = local_grads.reshape(NODES, D) + returned

    def back_one(carry, device):
        own_rows, averaged, norm_rows, sources, targets, before_relu = first(device)
        grad_rows = lax.dynamic_slice_in_dim(grad_hidden, (device * NODES_DEV).astype(jnp.int32), NODES_DEV, 0)
        grad_pre = jnp.where(before_relu > 0.0, grad_rows, 0.0).astype(jnp.bfloat16)
        grad_term = jnp.concatenate([
            jnp.einsum('rnd,ne->rde', averaged.astype(jnp.float32), grad_pre.astype(jnp.float32)),
            jnp.dot(own_rows.T, grad_pre, preferred_element_type=jnp.float32)[None]], axis=0)
        return carry + grad_term, None

    grad_one, unused = lax.scan(back_one, jnp.zeros((RELATIONS + 1, D, D), jnp.float32), devices)
    return (logits, loss, grad_one.reshape((RELATIONS + 1) * D, D), grad_two.reshape((RELATIONS + 1) * D, CLASSES))
```

```python
import functools

import jax
import jax.numpy as jnp
from jax import lax
from jax.experimental import pallas as pl
from jax.experimental.pallas import tpu as pltpu
from jax.sharding import PartitionSpec as P


loss_scale = 256.0
bf16 = jnp.bfloat16
f32 = jnp.float32
EXTRA = 128


def dot(a, b):
    return jnp.dot(a, b, preferred_element_type=f32)


def dot_nt(a, b):
    return lax.dot_general(a, b, (((1,), (1,)), ((), ())), preferred_element_type=f32)


def dot_tn(a, b):
    return lax.dot_general(a, b, (((0,), (0,)), ((), ())), preferred_element_type=f32)


def iota(shape, axis):
    return lax.broadcasted_iota(jnp.int32, shape, axis)


def call(body, outs, ins, scratch=(), flops=0, moved=0, smem=(), name=None, vmem=24):
    return pl.pallas_call(
        body,
        out_shape=[jax.ShapeDtypeStruct(s, d) for s, d in outs],
        in_specs=[
            pl.BlockSpec(memory_space=pltpu.SMEM if i in smem else pltpu.VMEM)
            for i in range(len(ins))
        ],
        out_specs=[pl.BlockSpec(memory_space=pltpu.VMEM) for _ in outs],
        scratch_shapes=list(scratch),
        compiler_params=pltpu.CompilerParams(vmem_limit_bytes=vmem << 20),
        cost_estimate=pl.CostEstimate(flops=flops, bytes_accessed=moved, transcendentals=0),
        name=name,
    )(*ins)


def pick_hot(slot_ref, rows):
    slots = slot_ref.shape[1]
    return jnp.where(iota((rows, slots), 0) == slot_ref[...], 1.0, 0.0).astype(bf16)


def pack_kernel(feat_ref, slot_ref, label_ref, out_ref):
    rows, width = feat_ref.shape
    slots = slot_ref.shape[1]
    out_ref[:, :width] = dot_tn(pick_hot(slot_ref, rows), feat_ref[...]).astype(bf16)
    count = jnp.sum(jnp.where(label_ref[...] >= 0, 1.0, 0.0), axis=1, keepdims=True)
    high = jnp.floor(count * (1.0 / 128.0))
    low = count - 128.0 * high
    lane = iota((slots, EXTRA), 1)
    out_ref[:, width:] = jnp.where(lane < 64, high, low).astype(bf16)


def graph_kernel(src_ref, dst_ref, adj_ref, back_ref, norm_ref):
    relations, blocks, edges = src_ref.shape
    table = adj_ref.shape[1]

    def step(r, carry):
        for b in range(blocks):
            start = pl.multiple_of((r * blocks + b) * 128, 128)
            src = src_ref[r, b : b + 1, :]
            dst = dst_ref[r, b : b + 1, :]
            hot_dst = jnp.where(iota((128, edges), 0) == dst, 1.0, 0.0)
            hot_src = jnp.where(iota((table, edges), 0) == src, 1.0, 0.0).astype(bf16)
            count = jnp.sum(hot_dst, axis=1, keepdims=True)
            hot_dst = hot_dst.astype(bf16)
            adj_ref[pl.ds(start, 128), :] = dot_nt(hot_dst, hot_src).astype(bf16)
            back_ref[:, pl.ds(start, 128)] = dot_nt(hot_src, hot_dst).astype(bf16)
            norm_ref[pl.ds(start, 128), :] = jnp.broadcast_to(
                1.0 / jnp.maximum(count, 1.0), (128, EXTRA)
            )
        return carry

    lax.fori_loop(0, relations, step, 0)


def wide(norm, width):
    return jnp.concatenate([norm] * (width // EXTRA), axis=1)


def first_kernel(adj_ref, norm_ref, feat_ref, got_ref, w_ref, slot_ref, avg_ref, hid_ref, pack_ref):
    rows, width = feat_ref.shape
    relations = w_ref.shape[0] - 1
    own = feat_ref[...]
    got = got_ref[:, :width]

    def step(r, total):
        at = pl.ds(pl.multiple_of(r * rows, rows), rows)
        sums = dot(adj_ref[at, :rows], own) + dot(adj_ref[at, rows:], got)
        avg = (sums * wide(norm_ref[at, :], width)).astype(bf16)
        avg_ref[at, :] = avg
        return total + dot(avg, w_ref[r])

    total = lax.fori_loop(0, relations, step, dot(own, w_ref[relations]))
    hidden = jnp.maximum(total, 0.0).astype(bf16)
    hid_ref[...] = hidden
    pack_ref[...] = dot_tn(pick_hot(slot_ref, rows), hidden).astype(bf16)


def second_kernel(
    adj_ref, back_ref, norm_ref, hid_ref, got_ref, w_ref, self_ref, label_ref, count_ref,
    logit_ref, avg_ref, grad_ref, spread_ref, out_ref, total_ref,
):
    rows, width = hid_ref.shape
    relations, _, classes = w_ref.shape
    own = hid_ref[...]
    got = got_ref[...]

    def step(r, total):
        at = pl.ds(pl.multiple_of(r * rows, rows), rows)
        sums = dot(adj_ref[at, :rows], own) + dot(adj_ref[at, rows:], got)
        avg = (sums * wide(norm_ref[at, :], width)).astype(bf16)
        avg_ref[at, :] = avg
        return total + dot(avg, w_ref[r])

    logits = lax.fori_loop(0, relations, step, dot(own, self_ref[...]))
    logit_ref[...] = logits

    counts = jnp.sum(count_ref[:, width:].astype(f32), axis=0, keepdims=True)
    count = (counts[:, 0:1] * 128.0 + counts[:, 64:65]) * 0.125
    labels = label_ref[...]
    labelled = jnp.where(labels >= 0, 1.0, 0.0)
    hot = jnp.where(iota((rows, classes), 1) == labels, 1.0, 0.0)
    peak = jnp.max(logits, axis=1, keepdims=True)
    log_total = peak + jnp.log(jnp.sum(jnp.exp(logits - peak), axis=1, keepdims=True))
    picked = jnp.sum(logits * hot, axis=1, keepdims=True)
    local = jnp.sum(jnp.where(labels >= 0, log_total - picked, 0.0), axis=0, keepdims=True)
    soft = jnp.exp(logits - log_total)
    grad = (loss_scale * (soft - hot) * labelled / count).astype(bf16)
    grad_ref[...] = grad
    total_ref[...] = jnp.broadcast_to(count, total_ref.shape)

    def spread_step(r, carry):
        at = pl.ds(pl.multiple_of(r * rows, rows), rows)
        spread = dot_nt(grad, w_ref[r]) * wide(norm_ref[at, :], width)
        spread_ref[at, :] = spread.astype(bf16)
        return carry

    lax.fori_loop(0, relations, spread_step, 0)
    slots = out_ref.shape[0]
    out_ref[:, :width] = dot(back_ref[rows:, :], spread_ref[...]).astype(bf16)
    first = local.astype(bf16).astype(f32)
    second = (local - first).astype(bf16).astype(f32)
    third = local - first - second
    lane = iota((slots, EXTRA), 1)
    out_ref[:, width:] = jnp.where(lane < 32, first, jnp.where(lane < 64, second, third)).astype(bf16)


def local_kernel(back_ref, spread_ref, grad_ref, self_ref, out_ref):
    rows = out_ref.shape[0]
    out_ref[...] = dot(back_ref[:rows, :], spread_ref[...]) + dot_nt(grad_ref[...], self_ref[...])


def turn_kernel(me_ref, avg_ref, own_ref, keep_ref, send_ref, scratch):
    rows, width = own_ref.shape
    parts = scratch.shape[0] // width
    places = keep_ref.shape[0] * 2
    block = scratch.shape[0] // places
    me = me_ref[0]
    for r in range(parts):
        value = own_ref[...] if r == parts - 1 else avg_ref[r * rows : (r + 1) * rows, :]
        scratch[r * width : (r + 1) * width, :] = value.T.astype(scratch.dtype)
    pad = keep_ref.shape[1] - block
    for b in range(places):
        place = jnp.bitwise_xor(me, b)
        half = jnp.right_shift(place, 1)
        value = scratch[b * block : (b + 1) * block, :].astype(bf16)
        if pad:
            value = jnp.concatenate([value, jnp.zeros((pad, rows), bf16)], axis=0)

        @pl.when(jnp.bitwise_and(place, 1) == 0)
        def _():
            keep_ref[half] = value

        @pl.when(jnp.bitwise_and(place, 1) == 1)
        def _():
            send_ref[half] = value


def grad_pre_kernel(slot_ref, got_ref, local_ref, hid_ref, count_ref, out_ref, loss_ref):
    rows, width = hid_ref.shape
    total = local_ref[...] + dot(pick_hot(slot_ref, rows), got_ref[:, :width])
    out_ref[...] = jnp.where(hid_ref[...].astype(f32) > 0.0, total, 0.0).astype(bf16)
    sums = jnp.sum(got_ref[:, width:].astype(f32), axis=0, keepdims=True)
    loss = (sums[:, 0:1] + sums[:, 32:33] + sums[:, 64:65]) * 0.125
    loss_ref[...] = loss / count_ref[:, 0:1]


class Colour:
    def __init__(self, start, size, order):
        self.start, self.size, self.order = start, size, order

    def places(self, stage):
        gone = self.order[:stage]
        bits = len(self.order)
        return [p for p in range(1 << bits) if not any(p >> g & 1 for g in gone)]

    def split(self, stage):
        bit = self.order[stage]
        here = self.places(stage)
        return [p for p in here if p >> bit & 1], [p for p in here if not p >> bit & 1]


def colours_of(bits, rows):
    tiles = rows // 16
    last = list(range(4, bits))
    orders = [[0, 1, 2, 3] + last, [1, 0, 2, 3] + last, [2, 3, 0, 1] + last]
    third = tiles * 2 // 9
    first = (tiles - third + 1) // 2
    sizes = [first, tiles - third - first, third]
    out, at = [], 0
    for size, order in zip(sizes, orders):
        if size:
            out.append(Colour(at * 16, size * 16, order))
        at += size
    return out


def product_kernel(colours, keep_ref, other_ref, grad_ref, other_grad_ref, *outs):
    grad, other_grad = grad_ref[...], other_grad_ref[...]
    width = grad.shape[1]
    for i, colour in enumerate(colours):
        rows = slice(colour.start, colour.start + colour.size)
        for places, out in zip(colour.split(0), outs[2 * i : 2 * i + 2]):
            left = jnp.concatenate([keep_ref[p, rows, :] for p in places], axis=0)
            right = jnp.concatenate([other_ref[p, rows, :] for p in places], axis=0)
            value = dot(left, grad) + dot(right, other_grad)
            out[...] = value.astype(out.dtype).reshape(len(places), colour.size, width)


def add_kernel(colours, stage, *refs):
    count = len(colours)
    ins, outs = refs[: 2 * count], refs[2 * count :]
    for i, colour in enumerate(colours):
        got, kept = ins[2 * i], ins[2 * i + 1]
        here = colour.places(stage)
        sent_places, kept_places = colour.split(stage)
        for places, out in zip((sent_places, kept_places), outs[2 * i : 2 * i + 2]):
            for j, p in enumerate(places):
                k = here.index(p)
                out[j] = (kept[k] + got[k].astype(f32)).astype(out.dtype)


def last_kernel(colours, block, *refs):
    out = refs[-1]
    for i, colour in enumerate(colours):
        got, kept = refs[2 * i], refs[2 * i + 1]
        size = min(colour.size, block - colour.start)
        if size > 0:
            value = kept[0] + got[0].astype(f32)
            out[colour.start : colour.start + size, :] = value[:size]


def across(value, bit):
    size = lax.axis_size("dom")
    return lax.ppermute(value, "dom", [(i, i ^ (2 << bit)) for i in range(size)])


def to_pair(value):
    size = lax.axis_size("dom")
    return lax.ppermute(value, "dom", [(i, i ^ 1) for i in range(size)])


def product(colours, keep, other, grad, other_grad, name):
    width = grad.shape[1]
    outs = []
    for colour in colours:
        sent, kept = colour.split(0)
        outs.append(((len(sent), colour.size, width), bf16))
        outs.append(((len(kept), colour.size, width), f32))
    ins = (keep, other, grad, other_grad)
    flops = 4 * keep.size * width
    return call(functools.partial(product_kernel, colours), outs, ins, flops=flops, moved=keep.size * 12, name=name)


def add_stage(colours, stage, got, kept, name):
    outs, ins = [], []
    for colour, g, k in zip(colours, got, kept):
        sent, keep = colour.split(stage)
        outs.append(((len(sent),) + g.shape[1:], bf16))
        outs.append(((len(keep),) + g.shape[1:], f32))
        ins += [g, k]
    size = sum(g.size for g in got)
    return call(functools.partial(add_kernel, colours, stage), outs, ins, flops=size * 200, moved=size * 10, name=name)


def finish(colours, block, got, kept, name):
    ins = []
    for g, k in zip(got, kept):
        ins += [g, k]
    outs = [((block, got[0].shape[2]), f32)]
    return call(functools.partial(last_kernel, colours, block), outs, ins, flops=block * 1000, moved=block * 5000, name=name)[0]


def scatter_sum(colours, block, parts, name):
    bits = len(colours[0].order)
    for stage in range(bits):
        sent, kept = parts[0::2], parts[1::2]
        got = [across(s, c.order[stage]) for s, c in zip(sent, colours)]
        if stage + 1 < bits:
            parts = add_stage(colours, stage + 1, got, kept, f"{name}_add{stage}")
    return finish(colours, block, got, kept, f"{name}_last")


def exchange(value):
    peers = lax.axis_size("dom")
    slots = value.shape[0] // peers
    cut = value.reshape(peers, slots, value.shape[1])
    return lax.all_to_all(cut, "dom", split_axis=0, concat_axis=0, tiled=True).reshape(value.shape)


def on_device(features, w_one, w_two, self_two, edge_src, edge_dst, send_rows, send_count, labels):
    peers = lax.axis_size("dom")
    rows, width = features.shape
    relations, _, classes = w_two.shape
    picks = send_rows[0]
    slots = picks.shape[1]
    boundary = peers * slots
    table = rows + boundary
    live = jnp.arange(slots, dtype=jnp.int32)[None, :] < send_count[0][:, None]
    slot = jnp.where(live, picks, -1).reshape(1, boundary)
    me = lax.axis_index("dom").astype(jnp.int32).reshape(1)
    all_rows = relations * rows
    block = (relations + 1) * width // peers
    padded = -(-block // 16) * 16
    bits = peers.bit_length() - 2
    colours = colours_of(bits, padded)
    turn_outs = [((peers // 2, padded, rows), bf16)] * 2
    turn_scratch = [pltpu.VMEM(((relations + 1) * width, rows), bf16 if block % 16 == 0 else f32)]

    packed, = call(
        pack_kernel, [((boundary, width + EXTRA), bf16)], (features, slot, labels.reshape(1, rows)),
        flops=2 * boundary * rows * width, moved=600000, name="pack",
    )
    got_one = exchange(packed)
    adj, back, norm = call(
        graph_kernel,
        [((all_rows, table), bf16), ((table, all_rows), bf16), ((all_rows, EXTRA), f32)],
        (edge_src, edge_dst), flops=4 * all_rows * 256 * table, moved=5 << 20, name="graph",
    )
    avg_one, hidden, packed = call(
        first_kernel,
        [((all_rows, width), bf16), ((rows, width), bf16), ((boundary, width), bf16)],
        (adj, norm, features, got_one, w_one, slot),
        flops=2 * all_rows * width * (table + width), moved=10 << 20, name="first",
    )
    got_two = exchange(packed)
    keep_one, send_one = call(
        turn_kernel, turn_outs, (me, avg_one, features), turn_scratch, smem=(0,),
        flops=1 << 30, moved=5 << 20, name="turn_one",
    )
    other_one = to_pair(send_one)
    logits, avg_two, grad_logits, spread, outgoing, count = call(
        second_kernel,
        [
            ((rows, classes), f32), ((all_rows, width), bf16), ((rows, classes), bf16),
            ((all_rows, width), bf16), ((boundary, width + EXTRA), bf16), ((1, EXTRA), f32),
        ],
        (adj, back, norm, hidden, got_two, w_two, self_two, labels.reshape(rows, 1), got_one),
        flops=8 * all_rows * width * width, moved=16 << 20, name="second", vmem=32,
    )
    returned = exchange(outgoing)
    keep_two, send_two = call(
        turn_kernel, turn_outs, (me, avg_two, hidden), turn_scratch, smem=(0,),
        flops=1 << 30, moved=5 << 20, name="turn_two",
    )
    other_two, other_logits = to_pair(send_two), to_pair(grad_logits)
    local, = call(
        local_kernel, [((rows, width), f32)], (back, spread, grad_logits, self_two),
        flops=2 * rows * all_rows * width, moved=4 << 20, name="local",
    )
    parts = product(colours, keep_two, other_two, grad_logits, other_logits, "product_two")
    grad_two = scatter_sum(colours, block, parts, "two")
    grad_pre, loss = call(
        grad_pre_kernel, [((rows, width), bf16), ((1, 1), f32)],
        (slot, returned, local, hidden, count),
        flops=2 * rows * boundary * width, moved=2 << 20, name="grad_pre",
    )
    other_pre = to_pair(grad_pre)
    parts = product(colours, keep_one, other_one, grad_pre, other_pre, "product_one")
    grad_one = scatter_sum(colours, block, parts, "one")
    return (logits, loss.reshape(()), grad_one, grad_two)


def solution(mesh):
    in_specs = (
        P("dom", None),
        P(),
        P(),
        P(),
        P(None, "dom", None),
        P(None, "dom", None),
        P("dom", None, None),
        P("dom", None),
        P("dom"),
    )
    out_specs = (P("dom", None), P(), P("dom", None), P("dom", None))
    return jax.shard_map(
        on_device, mesh=mesh, in_specs=in_specs, out_specs=out_specs, check_vma=False
    )
```

```python
import functools

import jax
import jax.numpy as jnp
from jax import lax
from jax.experimental import pallas as pl
from jax.experimental.pallas import tpu as pltpu
from jax.sharding import PartitionSpec as P


loss_scale = 256.0
bf16 = jnp.bfloat16
f32 = jnp.float32
EXTRA = 128


def dot(a, b):
    return jnp.dot(a, b, preferred_element_type=f32)


def dot_nt(a, b):
    return lax.dot_general(a, b, (((1,), (1,)), ((), ())), preferred_element_type=f32)


def dot_tn(a, b):
    return lax.dot_general(a, b, (((0,), (0,)), ((), ())), preferred_element_type=f32)


def iota(shape, axis):
    return lax.broadcasted_iota(jnp.int32, shape, axis)


HBM = pltpu.HBM
ALL_VMEM = 67043328


def call(body, outs, ins, spaces, out_spaces, scratch=(), copies=0, flops=0, moved=0, vmem=0):
    kinds = {"v": pltpu.VMEM, "h": pl.ANY, "s": pltpu.SMEM}
    out_kinds = {"v": pltpu.VMEM, "h": HBM}
    scratch = list(scratch)
    if copies:
        scratch.append(pltpu.SemaphoreType.DMA((copies,)))
    return pl.pallas_call(
        body,
        out_shape=[jax.ShapeDtypeStruct(s, d) for s, d in outs],
        in_specs=[pl.BlockSpec(memory_space=kinds[c]) for c in spaces],
        out_specs=[pl.BlockSpec(memory_space=out_kinds[c]) for c in out_spaces],
        scratch_shapes=scratch,
        compiler_params=pltpu.CompilerParams(vmem_limit_bytes=vmem << 20 or ALL_VMEM),
        cost_estimate=pl.CostEstimate(flops=flops, bytes_accessed=moved, transcendentals=0),
    )(*ins)


class Copies:
    def __init__(self, sems):
        self.sems, self.used = sems, 0

    def start(self, source, target):
        copy = pltpu.make_async_copy(source, target, self.sems.at[self.used])
        self.used += 1
        copy.start()
        return copy


def wait_all(copies):
    for copy in copies:
        copy.wait()


def pick_hot(picks, counts, rows):
    slots, peers = picks.shape
    chosen = jnp.where(iota((slots, peers), 0) < counts, picks, -1).astype(f32)
    lane = iota((peers, peers * slots), 1)
    spreader = jnp.where(iota((peers, peers * slots), 0) == lane // slots, 1.0, 0.0)
    laid = jnp.dot(chosen, spreader, preferred_element_type=f32, precision=lax.Precision.HIGHEST)
    mine = iota((slots, peers * slots), 0) == iota((slots, peers * slots), 1) % slots
    row = jnp.sum(jnp.where(mine, laid, 0.0), axis=0, keepdims=True)
    hot = iota((rows, peers * slots), 0) == jnp.round(row).astype(jnp.int32)
    return jnp.where(hot, 1.0, 0.0).astype(bf16)


def pack_kernel(feat_hbm, picks_hbm, count_hbm, label_hbm, out_ref, feat, picks, counts, label, sems):
    copies = Copies(sems)
    pairs = ((picks_hbm, picks), (count_hbm, counts), (label_hbm, label), (feat_hbm, feat))
    wait_all([copies.start(a, b) for a, b in pairs])
    rows, width = feat.shape
    slots = out_ref.shape[0]
    hot = pick_hot(picks[...], counts[...], rows)
    out_ref[:, :width] = dot_tn(hot, feat[...]).astype(bf16)
    count = jnp.sum(jnp.where(label[...] >= 0, 1.0, 0.0), axis=1, keepdims=True)
    high = jnp.floor(count * (1.0 / 128.0))
    low = count - 128.0 * high
    lane = iota((slots, EXTRA), 1)
    out_ref[:, width:] = jnp.where(lane < 64, high, low).astype(bf16)


def graph_kernel(
    src_hbm, dst_hbm, adj_hbm, norm_hbm, back_hbm, src_ref, dst_ref, adj_ref, norm_ref, back_ref, sems
):
    copies = Copies(sems)
    wait_all([copies.start(src_hbm, src_ref), copies.start(dst_hbm, dst_ref)])
    relations, blocks, edges = src_ref.shape
    table = adj_ref.shape[1]

    def step(r, carry):
        for b in range(blocks):
            start = pl.multiple_of((r * blocks + b) * 128, 128)
            src = src_ref[r, b : b + 1, :]
            dst = dst_ref[r, b : b + 1, :]
            hot_dst = jnp.where(iota((128, edges), 0) == dst, 1.0, 0.0)
            hot_src = jnp.where(iota((table, edges), 0) == src, 1.0, 0.0).astype(bf16)
            count = jnp.sum(hot_dst, axis=1, keepdims=True)
            hot_dst = hot_dst.astype(bf16)
            adj_ref[pl.ds(start, 128), :] = dot_nt(hot_dst, hot_src).astype(bf16)
            back_ref[:, pl.ds(start, 128)] = dot_nt(hot_src, hot_dst).astype(bf16)
            norm = 1.0 / jnp.maximum(count, 1.0)
            norm_ref[pl.ds(start, 128), :] = jnp.broadcast_to(norm, (128, EXTRA))
        return carry

    lax.fori_loop(0, relations, step, 0)
    pairs = ((adj_ref, adj_hbm), (norm_ref, norm_hbm), (back_ref, back_hbm))
    wait_all([copies.start(a, b) for a, b in pairs])


def wide(norm, width):
    return jnp.concatenate([norm] * (width // EXTRA), axis=1)


def put_blocks(me, turned, blocks, block):
    pad = blocks.shape[2] - block
    rows = blocks.shape[3]
    for b in range(turned.shape[0] // block):
        place = jnp.bitwise_xor(me, b)
        value = turned[b * block : (b + 1) * block, :].astype(bf16)
        if pad:
            value = jnp.concatenate([value, jnp.zeros((pad, rows), bf16)], axis=0)
        blocks[jnp.bitwise_and(place, 1), jnp.right_shift(place, 1)] = value


def first_kernel(
    adj_hbm, norm_hbm, got_hbm, feat_hbm, w_hbm, picks_hbm, count_hbm,
    left_hbm, hid_hbm, pack_hbm, total_hbm,
    adj, norm, got_ref, feat, w, picks, counts, left, hid, packed, total_ref, sems,
):
    copies = Copies(sems)
    rows, width = feat.shape
    relations = w.shape[0] // width - 1
    chunks = [slice(r * rows, (r + 2) * rows) for r in range(0, relations, 2)]
    near = [copies.start(feat_hbm, feat), copies.start(got_hbm, got_ref)]
    adj_in, norm_in, w_in = [], [], []
    for at in chunks:
        adj_in.append(copies.start(adj_hbm.at[at, :], adj.at[at, :]))
        norm_in.append(copies.start(norm_hbm.at[at, :], norm.at[at, :]))
    parts = [slice(0, 4 * width), slice(4 * width, 7 * width), slice(7 * width, (relations + 1) * width)]
    for at in parts:
        w_in.append(copies.start(w_hbm.at[at, :], w.at[at, :]))
    small = [copies.start(picks_hbm, picks), copies.start(count_hbm, counts)]
    wait_all(near)
    own = feat[...]
    got = got_ref[:, :width]
    left[:, relations * width :] = own
    for i, at in enumerate(chunks):
        adj_in[i].wait()
        norm_in[i].wait()
        sums = dot(adj[at, :rows], own) + dot(adj[at, rows:], got)
        avg = (sums * wide(norm[at, :], width)).astype(bf16)
        left[:, 2 * i * width : (2 * i + 1) * width] = avg[:rows]
        left[:, (2 * i + 1) * width : (2 * i + 2) * width] = avg[rows:]
    out = [copies.start(left, left_hbm)]
    wait_all(small)
    hot = pick_hot(picks[...], counts[...], rows)
    total = None
    for i, at in enumerate(parts):
        w_in[i].wait()
        part = dot(left[:, at], w[at, :])
        total = part if total is None else total + part
    hidden = jnp.maximum(total, 0.0).astype(bf16)
    packed[...] = dot_tn(hot, hidden).astype(bf16)
    out.append(copies.start(packed, pack_hbm))
    hid[...] = hidden
    out.append(copies.start(hid, hid_hbm))
    sums = jnp.sum(got_ref[:, width:].astype(f32), axis=0, keepdims=True)
    count = (sums[:, 0:1] * 128.0 + sums[:, 64:65]) * 0.125
    total_ref[...] = jnp.broadcast_to(count, total_ref.shape)
    out.append(copies.start(total_ref, total_hbm))
    wait_all(out)


def second_kernel(
    block, me_ref, got_hbm, adj_hbm, norm_hbm, back_hbm, hid_hbm, w_hbm, self_hbm, label_hbm, total_hbm,
    logit_hbm, keep_hbm, send_hbm, grad_hbm, local_hbm, out_hbm,
    got_ref, adj, norm, back, hid, w, selfs, label, total, logit, turned, blocks, grad_ref, spreads,
    local_ref, packed, sems,
):
    copies = Copies(sems)
    rows, width = hid.shape
    relations, classes, _ = w.shape
    chunks = [slice(r * rows, (r + 2) * rows) for r in range(0, relations, 2)]
    near = [copies.start(hid_hbm, hid), copies.start(got_hbm, got_ref)]
    adj_in, w_in, norm_in = [], [], []
    for i, at in enumerate(chunks):
        adj_in.append(copies.start(adj_hbm.at[at, :], adj.at[at, :]))
        norm_in.append(copies.start(norm_hbm.at[at, :], norm.at[at, :]))
        w_in.append(copies.start(w_hbm.at[2 * i : 2 * i + 2], w.at[2 * i : 2 * i + 2]))
    small = [copies.start(a, b) for a, b in ((self_hbm, selfs), (label_hbm, label), (total_hbm, total))]
    back_in = copies.start(back_hbm, back)
    wait_all(near)
    own = hid[...]
    got = got_ref[...]
    logits = None
    turned[relations * width :, :] = own.T.astype(turned.dtype)
    for i, at in enumerate(chunks):
        adj_in[i].wait()
        norm_in[i].wait()
        sums = dot(adj[at, :rows], own) + dot(adj[at, rows:], got)
        avg = (sums * wide(norm[at, :], width)).astype(bf16)
        w_in[i].wait()
        part = dot_nt(w[2 * i], avg[:rows]) + dot_nt(w[2 * i + 1], avg[rows:])
        logits = part if logits is None else logits + part
        for j in range(2):
            where = slice((2 * i + j) * width, (2 * i + j + 1) * width)
            turned[where, :] = avg[j * rows : (j + 1) * rows].T.astype(turned.dtype)
    wait_all(small)
    logits = logits + dot_nt(selfs[...], own)
    logit[...] = logits
    out = [copies.start(logit, logit_hbm)]
    put_blocks(me_ref[0], turned, blocks, block)
    out += [copies.start(blocks.at[0], keep_hbm), copies.start(blocks.at[1], send_hbm)]
    count = total[0:1, 0:1]
    labels = label[...]
    labelled = jnp.where(labels >= 0, 1.0, 0.0)
    hot = jnp.where(iota((classes, rows), 0) == labels, 1.0, 0.0)
    peak = jnp.max(logits, axis=0, keepdims=True)
    log_total = peak + jnp.log(jnp.sum(jnp.exp(logits - peak), axis=0, keepdims=True))
    picked = jnp.sum(logits * hot, axis=0, keepdims=True)
    local = jnp.sum(jnp.where(labels >= 0, log_total - picked, 0.0), axis=1, keepdims=True)
    soft = jnp.exp(logits - log_total)
    grad = (loss_scale * (soft - hot) * labelled / count).T.astype(bf16)
    grad_ref[...] = grad
    out.append(copies.start(grad_ref, grad_hbm))
    for r in range(relations):
        at = slice(r * rows, (r + 1) * rows)
        spread = dot(grad, w[r]) * wide(norm[at, :], width)
        spreads[at, :] = spread.astype(bf16)
    slots = packed.shape[0]
    first = local.astype(bf16).astype(f32)
    second = (local - first).astype(bf16).astype(f32)
    third = local - first - second
    lane = iota((slots, EXTRA), 1)
    packed[:, width:] = jnp.where(lane < 32, first, jnp.where(lane < 64, second, third)).astype(bf16)
    back_in.wait()
    packed[:, :width] = dot(back[rows:, :], spreads[...]).astype(bf16)
    out.append(copies.start(packed, out_hbm))
    local_ref[...] = dot(back[:rows, :], spreads[...]) + dot(grad, selfs[...])
    out.append(copies.start(local_ref, local_hbm))
    wait_all(out)


def turn_kernel(block, me_ref, left_hbm, keep_hbm, send_hbm, left, turned, blocks, sems):
    copies = Copies(sems)
    step = turned.shape[0] // 3
    cuts = [slice(i * step, (i + 1) * step) for i in range(3)]
    ins = [copies.start(left_hbm.at[:, at], left.at[:, at]) for at in cuts]
    for at, copy in zip(cuts, ins):
        copy.wait()
        turned[at, :] = left[:, at].T.astype(turned.dtype)
    put_blocks(me_ref[0], turned, blocks, block)
    wait_all([copies.start(blocks.at[0], keep_hbm), copies.start(blocks.at[1], send_hbm)])


def grad_pre_kernel(
    got_ref, local_ref, after_ref, picks_hbm, count_hbm, hid_hbm, total_hbm, out_ref, loss_ref,
    picks, counts, hid, total, sems,
):
    copies = Copies(sems)
    pairs = ((picks_hbm, picks), (count_hbm, counts), (hid_hbm, hid), (total_hbm, total))
    wait_all([copies.start(a, b) for a, b in pairs])
    rows, width = hid.shape
    grad = local_ref[...] + dot(pick_hot(picks[...], counts[...], rows), got_ref[:, :width])
    out_ref[...] = jnp.where(hid[...].astype(f32) > 0.0, grad, 0.0).astype(bf16)
    sums = jnp.sum(got_ref[:, width:].astype(f32), axis=0, keepdims=True)
    loss = (sums[:, 0:1] + sums[:, 32:33] + sums[:, 64:65]) * 0.125
    loss_ref[...] = loss / total[0:1, 0:1]


class Colour:
    def __init__(self, start, size, order):
        self.start, self.size, self.order = start, size, order

    def places(self, stage):
        gone = self.order[:stage]
        bits = len(self.order)
        return [p for p in range(1 << bits) if not any(p >> g & 1 for g in gone)]

    def split(self, stage):
        bit = self.order[stage]
        here = self.places(stage)
        return [p for p in here if p >> bit & 1], [p for p in here if not p >> bit & 1]


def colours_of(bits, rows):
    tiles = rows // 16
    last = list(range(4, bits))
    orders = [[0, 2, 1, 3] + last, [1, 0, 2, 3] + last, [2, 1, 3, 0] + last]
    third = tiles // 3
    sizes = [tiles - 2 * third, third, third]
    out, at = [], 0
    for size, order in zip(sizes, orders):
        if size:
            out.append(Colour(at * 16, size * 16, order))
        at += size
    return out


def product_kernel(colours, keep_hbm, other_hbm, grad_ref, other_grad_ref, *refs):
    outs, (keep, other, sems) = refs[: 2 * len(colours)], refs[2 * len(colours) :]
    copies = Copies(sems)
    ins = []
    for colour in colours:
        rows = slice(colour.start, colour.start + colour.size)
        ins.append(copies.start(keep_hbm.at[:, rows, :], keep.at[:, rows, :]))
        ins.append(copies.start(other_hbm.at[:, rows, :], other.at[:, rows, :]))
    grad, other_grad = grad_ref[...], other_grad_ref[...]
    width = grad.shape[1]
    for i, colour in enumerate(colours):
        rows = slice(colour.start, colour.start + colour.size)
        wait_all(ins[2 * i : 2 * i + 2])
        for places, out in zip(colour.split(0), outs[2 * i : 2 * i + 2]):
            left = jnp.concatenate([keep[p, rows, :] for p in places], axis=0)
            right = jnp.concatenate([other[p, rows, :] for p in places], axis=0)
            value = dot(left, grad) + dot(right, other_grad)
            out[...] = value.astype(out.dtype).reshape(len(places), colour.size, width)


def add_kernel(colour, stage, got, kept, *outs):
    here = colour.places(stage)
    for places, out in zip(colour.split(stage), outs):
        for j, p in enumerate(places):
            k = here.index(p)
            out[j] = (kept[k] + got[k].astype(f32)).astype(out.dtype)


def last_kernel(colours, block, *refs):
    out = refs[-1]
    for i, colour in enumerate(colours):
        got, kept = refs[2 * i], refs[2 * i + 1]
        size = min(colour.size, block - colour.start)
        if size > 0:
            value = kept[0] + got[0].astype(f32)
            out[colour.start : colour.start + size, :] = value[:size]


def across(value, bit):
    size = lax.axis_size("dom")
    return lax.ppermute(value, "dom", [(i, i ^ (2 << bit)) for i in range(size)])


def to_pair(value):
    size = lax.axis_size("dom")
    return lax.ppermute(value, "dom", [(i, i ^ 1) for i in range(size)])


def product(colours, keep, other, grad, other_grad):
    width = grad.shape[1]
    outs = []
    for colour in colours:
        sent, kept = colour.split(0)
        outs.append(((len(sent), colour.size, width), bf16))
        outs.append(((len(kept), colour.size, width), f32))
    ins = (keep, other, grad, other_grad)
    return call(
        functools.partial(product_kernel, colours), outs, ins, "hhvv", "v" * len(outs),
        [pltpu.VMEM(keep.shape, bf16)] * 2, 2 * len(colours),
        flops=4 * keep.size * width, moved=keep.size * 12, vmem=16,
    )


def add_stage(colour, stage, got, kept):
    sent, keep = colour.split(stage)
    outs = [((len(sent),) + got.shape[1:], bf16), ((len(keep),) + got.shape[1:], f32)]
    return call(
        functools.partial(add_kernel, colour, stage), outs, (got, kept), "vv", "vv",
        flops=got.size * 200, moved=got.size * 10, vmem=4,
    )


def scatter_sum(colours, block, parts):
    bits = len(colours[0].order)
    ends = []
    states = [list(parts[2 * i : 2 * i + 2]) for i in range(len(colours))]
    for stage in range(bits):
        for i, colour in enumerate(colours):
            sent, kept = states[i]
            got = across(sent, colour.order[stage])
            if stage + 1 < bits:
                states[i] = add_stage(colour, stage + 1, got, kept)
            else:
                ends += [got, kept]
    return call(
        functools.partial(last_kernel, colours, block), [((block, ends[0].shape[2]), f32)], ends,
        "v" * len(ends), "v", flops=block * 1000, moved=block * 5000, vmem=4,
    )[0]


def exchange(value):
    peers = lax.axis_size("dom")
    slots = value.shape[0] // peers
    cut = value.reshape(peers, slots, value.shape[1])
    got = lax.all_to_all(cut, "dom", split_axis=0, concat_axis=0, tiled=True)
    return got.reshape(value.shape)


def on_device(features, w_one, w_two, self_two, edge_src, edge_dst, send_rows, send_count, labels):
    peers = lax.axis_size("dom")
    rows, width = features.shape
    relations, _, classes = w_two.shape
    blocks, edges = edge_src.shape[1:]
    picks = send_rows[0].T
    slots = picks.shape[0]
    boundary = peers * slots
    table = rows + boundary
    label_row = labels.reshape(1, rows)
    me = lax.axis_index("dom").astype(jnp.int32).reshape(1)
    all_rows = relations * rows
    block = (relations + 1) * width // peers
    padded = -(-block // 16) * 16
    bits = peers.bit_length() - 2
    colours = colours_of(bits, padded)
    w_two = jnp.swapaxes(w_two, 1, 2)
    self_two = self_two.T

    vm = pltpu.VMEM
    picks_vm, counts_vm = vm((slots, peers), jnp.int32), vm((1, peers), jnp.int32)
    own_vm, total_vm = vm((rows, width), bf16), vm((8, EXTRA), f32)
    adj_vm, norm_vm = vm((all_rows, table), bf16), vm((all_rows, EXTRA), f32)
    back_vm = vm((table, all_rows), bf16)
    edge_vm = vm((relations, blocks, edges), jnp.int32)
    deep = (relations + 1) * width
    left_vm = vm((rows, deep), bf16)
    turned_vm = vm((deep, rows), bf16 if block % 16 == 0 else f32)
    blocks_vm = vm((2, peers // 2, padded, rows), bf16)
    turn_outs = [((peers // 2, padded, rows), bf16)] * 2
    packed_vm = vm((boundary, width + EXTRA), bf16)

    packed, = call(
        pack_kernel, [((boundary, width + EXTRA), bf16)], (features, picks, send_count, label_row),
        "hhhh", "v", [own_vm, picks_vm, counts_vm, vm((1, rows), jnp.int32)], 4,
        flops=2 * boundary * rows * width, moved=600000,
    )
    got_one = exchange(packed)
    adj, norm, back = call(
        graph_kernel,
        [((all_rows, table), bf16), ((all_rows, EXTRA), f32), ((table, all_rows), bf16)],
        (edge_src, edge_dst), "hh", "hhh", [edge_vm] * 2 + [adj_vm, norm_vm, back_vm], 5,
        flops=4 * all_rows * 256 * table, moved=5 << 20,
    )
    left_one, hidden, packed, total = call(
        first_kernel,
        [((rows, deep), bf16), ((rows, width), bf16), ((boundary, width), bf16), ((8, EXTRA), f32)],
        (adj, norm, got_one, features, w_one.reshape(deep, width), picks, send_count), "hhhhhhh", "hhhh",
        [
            adj_vm, norm_vm, packed_vm, own_vm, vm((deep, width), bf16), picks_vm, counts_vm, left_vm,
            own_vm, vm((boundary, width), bf16), total_vm,
        ],
        7 + relations + 4,
        flops=2 * all_rows * width * (table + width), moved=10 << 20,
    )
    got_two = exchange(packed)
    keep_one, send_one = call(
        functools.partial(turn_kernel, block), turn_outs, (me, left_one), "sh", "hh",
        [left_vm, turned_vm, blocks_vm], 5, flops=1 << 30, moved=5 << 20,
    )
    other_one = to_pair(send_one)
    logits, keep_two, send_two, grad_logits, local, outgoing = call(
        functools.partial(second_kernel, block),
        [((classes, rows), f32)] + turn_outs
        + [((rows, classes), bf16), ((rows, width), f32), ((boundary, width + EXTRA), bf16)],
        (me, got_two, adj, norm, back, hidden, w_two, self_two, label_row, total), "shhhhhhhhh", "hhhhhh",
        [
            vm((boundary, width), bf16), adj_vm, norm_vm, back_vm, own_vm, vm(w_two.shape, bf16),
            vm(self_two.shape, bf16), vm((1, rows), jnp.int32), total_vm, vm((classes, rows), f32),
            turned_vm, blocks_vm, vm((rows, classes), bf16), vm((all_rows, width), bf16),
            vm((rows, width), f32), packed_vm,
        ],
        2 + 3 * (relations // 2) + 4 + 6,
        flops=8 * all_rows * width * width, moved=16 << 20,
    )
    other_two, other_logits = to_pair(send_two), to_pair(grad_logits)
    returned = exchange(outgoing)
    parts_two = product(colours, keep_two, other_two, grad_logits, other_logits)
    grad_pre, loss = call(
        grad_pre_kernel, [((rows, width), bf16), ((1, 1), f32)],
        (returned, local, parts_two[0], picks, send_count, hidden, total), "vvhhhhh", "vv",
        [picks_vm, counts_vm, own_vm, total_vm], 4,
        flops=2 * rows * boundary * width, moved=2 << 20, vmem=50,
    )
    other_pre = to_pair(grad_pre)
    parts_one = product(colours, keep_one, other_one, grad_pre, other_pre)
    grad_two = scatter_sum(colours, block, parts_two)
    grad_one = scatter_sum(colours, block, parts_one)
    return (logits.T, loss.reshape(()), grad_one, grad_two)


def solution(mesh):
    in_specs = (
        P("dom", None),
        P(),
        P(),
        P(),
        P(None, "dom", None),
        P(None, "dom", None),
        P("dom", None, None),
        P("dom", None),
        P("dom"),
    )
    out_specs = (P("dom", None), P(), P("dom", None), P("dom", None))
    return jax.shard_map(on_device, mesh=mesh, in_specs=in_specs, out_specs=out_specs, check_vma=False)
```

```python
import functools

import jax
import jax.numpy as jnp
from jax import lax
from jax.experimental import pallas as pl
from jax.experimental.pallas import tpu as pltpu
from jax.sharding import PartitionSpec as P


loss_scale = 256.0
bf16 = jnp.bfloat16
f32 = jnp.float32
EXTRA = 128


def dot(a, b):
    return jnp.dot(a, b, preferred_element_type=f32)


def dot_nt(a, b):
    return lax.dot_general(a, b, (((1,), (1,)), ((), ())), preferred_element_type=f32)


def dot_tn(a, b):
    return lax.dot_general(a, b, (((0,), (0,)), ((), ())), preferred_element_type=f32)


def iota(shape, axis):
    return lax.broadcasted_iota(jnp.int32, shape, axis)


def call(body, outs, ins, spaces, out_spaces, scratch=(), copies=0, flops=0, moved=0, vmem=32):
    kinds = {"v": pltpu.VMEM, "V": pltpu.VMEM, "H": pltpu.VMEM, "h": pl.ANY, "s": pltpu.SMEM}
    kept = {"h": pltpu.HBM, "H": pltpu.HBM, "V": pltpu.VMEM}
    scratch = list(scratch)
    if copies:
        scratch.append(pltpu.SemaphoreType.DMA((copies,)))
    ins = [pltpu.with_memory_space_constraint(x, kept[c]) if c in kept else x for x, c in zip(ins, spaces)]
    return pl.pallas_call(
        body,
        out_shape=[kept[c](s, d) if c in kept else jax.ShapeDtypeStruct(s, d) for (s, d), c in zip(outs, out_spaces)],
        in_specs=[pl.BlockSpec(memory_space=kinds[c]) for c in spaces],
        out_specs=[pl.BlockSpec(memory_space=kinds[c]) for c in out_spaces],
        scratch_shapes=scratch,
        compiler_params=pltpu.CompilerParams(vmem_limit_bytes=vmem << 20),
        cost_estimate=pl.CostEstimate(flops=flops, bytes_accessed=moved, transcendentals=0),
    )(*ins)


class Copies:
    def __init__(self, sems):
        self.sems, self.used = sems, 0

    def start(self, source, target):
        copy = pltpu.make_async_copy(source, target, self.sems.at[self.used])
        self.used += 1
        copy.start()
        return copy


def wait_all(copies):
    for copy in copies:
        copy.wait()


def pick_hot(picks, counts, rows):
    slots, peers = picks.shape
    chosen = jnp.where(iota((slots, peers), 0) < counts, picks, -1).astype(f32)
    lane = iota((peers, peers * slots), 1)
    spreader = jnp.where(iota((peers, peers * slots), 0) == lane // slots, 1.0, 0.0)
    laid = jnp.dot(chosen, spreader, preferred_element_type=f32, precision=lax.Precision.HIGHEST)
    mine = iota((slots, peers * slots), 0) == iota((slots, peers * slots), 1) % slots
    row = jnp.sum(jnp.where(mine, laid, 0.0), axis=0, keepdims=True)
    hot = iota((rows, peers * slots), 0) == jnp.round(row).astype(jnp.int32)
    return jnp.where(hot, 1.0, 0.0).astype(bf16)


def pack_kernel(feat_hbm, picks_hbm, count_hbm, label_hbm, out_ref, feat, picks, counts, label, sems):
    copies = Copies(sems)
    pairs = ((picks_hbm, picks), (count_hbm, counts), (label_hbm, label), (feat_hbm, feat))
    wait_all([copies.start(a, b) for a, b in pairs])
    rows, width = feat.shape
    slots = out_ref.shape[0]
    hot = pick_hot(picks[...], counts[...], rows)
    out_ref[:, :width] = dot_tn(hot, feat[...]).astype(bf16)
    count = jnp.sum(jnp.where(label[...] >= 0, 1.0, 0.0), axis=1, keepdims=True)
    high = jnp.floor(count * (1.0 / 128.0))
    low = count - 128.0 * high
    lane = iota((slots, EXTRA), 1)
    out_ref[:, width:] = jnp.where(lane < 64, high, low).astype(bf16)


def graph_kernel(
    src_hbm, dst_hbm, adj_ref, norm_ref, back_hbm, src_ref, dst_ref, back_ref, sems
):
    copies = Copies(sems)
    wait_all([copies.start(src_hbm, src_ref), copies.start(dst_hbm, dst_ref)])
    relations, blocks, edges = src_ref.shape
    table = adj_ref.shape[1]

    def step(r, carry):
        for b in range(blocks):
            start = pl.multiple_of((r * blocks + b) * 128, 128)
            src = src_ref[r, b : b + 1, :]
            dst = dst_ref[r, b : b + 1, :]
            hot_dst = jnp.where(iota((128, edges), 0) == dst, 1.0, 0.0)
            hot_src = jnp.where(iota((table, edges), 0) == src, 1.0, 0.0).astype(bf16)
            count = jnp.sum(hot_dst, axis=1, keepdims=True)
            hot_dst = hot_dst.astype(bf16)
            adj_ref[pl.ds(start, 128), :] = dot_nt(hot_dst, hot_src).astype(bf16)
            back_ref[:, pl.ds(start, 128)] = dot_nt(hot_src, hot_dst).astype(bf16)
            norm = 1.0 / jnp.maximum(count, 1.0)
            norm_ref[pl.ds(start, 128), :] = jnp.broadcast_to(norm, (128, EXTRA))
        return carry

    lax.fori_loop(0, relations, step, 0)
    copies.start(back_ref, back_hbm).wait()


def wide(norm, width):
    return jnp.concatenate([norm] * (width // EXTRA), axis=1)


def put_blocks(me, turned, blocks, block):
    pad = blocks.shape[2] - block
    rows = blocks.shape[3]
    for b in range(turned.shape[0] // block):
        place = jnp.bitwise_xor(me, b)
        value = turned[b * block : (b + 1) * block, :].astype(bf16)
        if pad:
            value = jnp.concatenate([value, jnp.zeros((pad, rows), bf16)], axis=0)
        blocks[jnp.bitwise_and(place, 1), jnp.right_shift(place, 1)] = value


def first_kernel(
    adj, norm, got_ref, feat_hbm, w_hbm, picks_hbm, count_hbm,
    left_hbm, hid_hbm, pack_hbm, total_hbm,
    feat, w, picks, counts, left, hid, packed, total_ref, sems,
):
    copies = Copies(sems)
    rows, width = feat.shape
    relations = w.shape[0] // width - 1
    chunks = [slice(r * rows, (r + 2) * rows) for r in range(0, relations, 2)]
    near = [copies.start(feat_hbm, feat)]
    w_in = []
    parts = [slice(0, 4 * width), slice(4 * width, 7 * width), slice(7 * width, (relations + 1) * width)]
    for at in parts:
        w_in.append(copies.start(w_hbm.at[at, :], w.at[at, :]))
    small = [copies.start(picks_hbm, picks), copies.start(count_hbm, counts)]
    wait_all(near)
    own = feat[...]
    got = got_ref[:, :width]
    left[:, relations * width :] = own
    for i, at in enumerate(chunks):
        sums = dot(adj[at, :rows], own) + dot(adj[at, rows:], got)
        avg = (sums * wide(norm[at, :], width)).astype(bf16)
        left[:, 2 * i * width : (2 * i + 1) * width] = avg[:rows]
        left[:, (2 * i + 1) * width : (2 * i + 2) * width] = avg[rows:]
    out = [copies.start(left, left_hbm)]
    wait_all(small)
    hot = pick_hot(picks[...], counts[...], rows)
    total = None
    for i, at in enumerate(parts):
        w_in[i].wait()
        part = dot(left[:, at], w[at, :])
        total = part if total is None else total + part
    hidden = jnp.maximum(total, 0.0).astype(bf16)
    packed[...] = dot_tn(hot, hidden).astype(bf16)
    out.append(copies.start(packed, pack_hbm))
    hid[...] = hidden
    out.append(copies.start(hid, hid_hbm))
    sums = jnp.sum(got_ref[:, width:].astype(f32), axis=0, keepdims=True)
    count = (sums[:, 0:1] * 128.0 + sums[:, 64:65]) * 0.125
    total_ref[...] = jnp.broadcast_to(count, total_ref.shape)
    out.append(copies.start(total_ref, total_hbm))
    wait_all(out)


def second_kernel(
    block, me_ref, got_ref, adj, norm, back_hbm, hid_hbm, w_hbm, self_hbm, label_hbm, total_hbm,
    logit_hbm, keep_hbm, send_hbm, grad_hbm, local_hbm, out_hbm,
    back, hid, w, selfs, label, total, logit, turned, blocks, grad_ref, spreads,
    local_ref, packed, sems,
):
    copies = Copies(sems)
    rows, width = hid.shape
    relations, classes, _ = w.shape
    chunks = [slice(r * rows, (r + 2) * rows) for r in range(0, relations, 2)]
    near = [copies.start(hid_hbm, hid)]
    w_in = []
    for i in range(len(chunks)):
        w_in.append(copies.start(w_hbm.at[2 * i : 2 * i + 2], w.at[2 * i : 2 * i + 2]))
    small = [copies.start(a, b) for a, b in ((self_hbm, selfs), (label_hbm, label), (total_hbm, total))]
    back_in = copies.start(back_hbm, back)
    wait_all(near)
    own = hid[...]
    got = got_ref[...]
    logits = None
    turned[relations * width :, :] = own.T.astype(turned.dtype)
    for i, at in enumerate(chunks):
        sums = dot(adj[at, :rows], own) + dot(adj[at, rows:], got)
        avg = (sums * wide(norm[at, :], width)).astype(bf16)
        w_in[i].wait()
        part = dot_nt(w[2 * i], avg[:rows]) + dot_nt(w[2 * i + 1], avg[rows:])
        logits = part if logits is None else logits + part
        for j in range(2):
            where = slice((2 * i + j) * width, (2 * i + j + 1) * width)
            turned[where, :] = avg[j * rows : (j + 1) * rows].T.astype(turned.dtype)
    wait_all(small)
    logits = logits + dot_nt(selfs[...], own)
    logit[...] = logits
    out = [copies.start(logit, logit_hbm)]
    put_blocks(me_ref[0], turned, blocks, block)
    out += [copies.start(blocks.at[0], keep_hbm), copies.start(blocks.at[1], send_hbm)]
    count = total[0:1, 0:1]
    labels = label[...]
    labelled = jnp.where(labels >= 0, 1.0, 0.0)
    hot = jnp.where(iota((classes, rows), 0) == labels, 1.0, 0.0)
    peak = jnp.max(logits, axis=0, keepdims=True)
    log_total = peak + jnp.log(jnp.sum(jnp.exp(logits - peak), axis=0, keepdims=True))
    picked = jnp.sum(logits * hot, axis=0, keepdims=True)
    local = jnp.sum(jnp.where(labels >= 0, log_total - picked, 0.0), axis=1, keepdims=True)
    soft = jnp.exp(logits - log_total)
    grad = (loss_scale * (soft - hot) * labelled / count).T.astype(bf16)
    grad_ref[...] = grad
    out.append(copies.start(grad_ref, grad_hbm))
    for r in range(relations):
        at = slice(r * rows, (r + 1) * rows)
        spread = dot(grad, w[r]) * wide(norm[at, :], width)
        spreads[at, :] = spread.astype(bf16)
    slots = packed.shape[0]
    first = local.astype(bf16).astype(f32)
    second = (local - first).astype(bf16).astype(f32)
    third = local - first - second
    lane = iota((slots, EXTRA), 1)
    packed[:, width:] = jnp.where(lane < 32, first, jnp.where(lane < 64, second, third)).astype(bf16)
    back_in.wait()
    packed[:, :width] = dot(back[rows:, :], spreads[...]).astype(bf16)
    out.append(copies.start(packed, out_hbm))
    local_ref[...] = dot(back[:rows, :], spreads[...]) + dot(grad, selfs[...])
    out.append(copies.start(local_ref, local_hbm))
    wait_all(out)


def turn_kernel(block, me_ref, left_hbm, keep_hbm, send_hbm, left, turned, blocks, sems):
    copies = Copies(sems)
    step = turned.shape[0] // 3
    cuts = [slice(i * step, (i + 1) * step) for i in range(3)]
    ins = [copies.start(left_hbm.at[:, at], left.at[:, at]) for at in cuts]
    for at, copy in zip(cuts, ins):
        copy.wait()
        turned[at, :] = left[:, at].T.astype(turned.dtype)
    put_blocks(me_ref[0], turned, blocks, block)
    wait_all([copies.start(blocks.at[0], keep_hbm), copies.start(blocks.at[1], send_hbm)])


def grad_pre_kernel(
    got_ref, after_ref, local_hbm, hid_hbm, picks_hbm, count_hbm, total_hbm,
    out_ref, loss_ref, local, hid, picks, counts, total, sems,
):
    copies = Copies(sems)
    pairs = (
        (picks_hbm, picks), (count_hbm, counts), (local_hbm, local), (hid_hbm, hid), (total_hbm, total),
    )
    ins = [copies.start(a, b) for a, b in pairs]
    wait_all(ins[:2])
    rows, width = local.shape
    grad = dot(pick_hot(picks[...], counts[...], rows), got_ref[:, :width])
    sums = jnp.sum(got_ref[:, width:].astype(f32), axis=0, keepdims=True)
    loss = (sums[:, 0:1] + sums[:, 32:33] + sums[:, 64:65]) * 0.125
    wait_all(ins[2:])
    out_ref[...] = jnp.where(hid[...].astype(f32) > 0.0, local[...] + grad, 0.0).astype(bf16)
    loss_ref[...] = loss / total[0:1, 0:1]


def bring_kernel(*refs):
    count = len(refs) // 2
    copies = Copies(refs[-1])
    wait_all([copies.start(a, b) for a, b in zip(refs[:count], refs[count : 2 * count])])


class Colour:
    def __init__(self, start, size, order):
        self.start, self.size, self.order = start, size, order

    def places(self, stage):
        gone = self.order[:stage]
        bits = len(self.order)
        return [p for p in range(1 << bits) if not any(p >> g & 1 for g in gone)]

    def split(self, stage):
        bit = self.order[stage]
        here = self.places(stage)
        return [p for p in here if p >> bit & 1], [p for p in here if not p >> bit & 1]


def colours_of(bits, rows):
    tiles = rows // 16
    last = list(range(4, bits))
    orders = [[0, 2, 1, 3] + last, [1, 0, 2, 3] + last, [2, 1, 3, 0] + last]
    third = tiles // 3
    sizes = [tiles - 2 * third, third, third]
    out, at = [], 0
    for size, order in zip(sizes, orders):
        if size:
            out.append(Colour(at * 16, size * 16, order))
        at += size
    return out


def product_kernel(colours, keep_ref, other_ref, grad_ref, other_grad_ref, *outs):
    grad, other_grad = grad_ref[...], other_grad_ref[...]
    width = grad.shape[1]
    for i, colour in enumerate(colours):
        rows = slice(colour.start, colour.start + colour.size)
        for places, out in zip(colour.split(0), outs[2 * i : 2 * i + 2]):
            left = jnp.concatenate([keep_ref[p, rows, :] for p in places], axis=0)
            right = jnp.concatenate([other_ref[p, rows, :] for p in places], axis=0)
            value = dot(left, grad) + dot(right, other_grad)
            out[...] = value.astype(out.dtype).reshape(len(places), colour.size, width)


def add_kernel(colour, stage, got, kept, *outs):
    here = colour.places(stage)
    for places, out in zip(colour.split(stage), outs):
        for j, p in enumerate(places):
            k = here.index(p)
            out[j] = (kept[k] + got[k].astype(f32)).astype(out.dtype)


def last_kernel(colours, block, *refs):
    out = refs[-1]
    for i, colour in enumerate(colours):
        got, kept = refs[2 * i], refs[2 * i + 1]
        size = min(colour.size, block - colour.start)
        if size > 0:
            value = kept[0] + got[0].astype(f32)
            out[colour.start : colour.start + size, :] = value[:size]


def across(value, bit):
    size = lax.axis_size("dom")
    return lax.ppermute(value, "dom", [(i, i ^ (2 << bit)) for i in range(size)])


def to_pair(value):
    size = lax.axis_size("dom")
    return lax.ppermute(value, "dom", [(i, i ^ 1) for i in range(size)])


def product(colours, keep, other, grad, other_grad, spaces):
    width = grad.shape[1]
    outs = []
    for colour in colours:
        sent, kept = colour.split(0)
        outs.append(((len(sent), colour.size, width), bf16))
        outs.append(((len(kept), colour.size, width), f32))
    ins = (keep, other, grad, other_grad)
    return call(
        functools.partial(product_kernel, colours), outs, ins, "vvvv", spaces * len(colours),
        flops=4 * keep.size * width, moved=keep.size * 12, vmem=16,
    )


def add_stage(colour, stage, got, kept):
    sent, keep = colour.split(stage)
    outs = [((len(sent),) + got.shape[1:], bf16), ((len(keep),) + got.shape[1:], f32)]
    return call(
        functools.partial(add_kernel, colour, stage), outs, (got, kept), "vv", "vv",
        flops=got.size * 200, moved=got.size * 10, vmem=4,
    )


def scatter_sum(colours, block, parts):
    bits = len(colours[0].order)
    ends = []
    states = [list(parts[2 * i : 2 * i + 2]) for i in range(len(colours))]
    for stage in range(bits):
        for i, colour in enumerate(colours):
            sent, kept = states[i]
            got = across(sent, colour.order[stage])
            if stage + 1 < bits:
                states[i] = add_stage(colour, stage + 1, got, kept)
            else:
                ends += [got, kept]
    return call(
        functools.partial(last_kernel, colours, block), [((block, ends[0].shape[2]), f32)], ends,
        "v" * len(ends), "v", flops=block * 1000, moved=block * 5000, vmem=4,
    )[0]


def exchange(value):
    peers = lax.axis_size("dom")
    slots = value.shape[0] // peers
    cut = value.reshape(peers, slots, value.shape[1])
    got = lax.all_to_all(cut, "dom", split_axis=0, concat_axis=0, tiled=True)
    return got.reshape(value.shape)


def on_device(features, w_one, w_two, self_two, edge_src, edge_dst, send_rows, send_count, labels):
    peers = lax.axis_size("dom")
    rows, width = features.shape
    relations, _, classes = w_two.shape
    blocks, edges = edge_src.shape[1:]
    picks = send_rows[0].T
    slots = picks.shape[0]
    boundary = peers * slots
    table = rows + boundary
    label_row = labels.reshape(1, rows)
    me = lax.axis_index("dom").astype(jnp.int32).reshape(1)
    all_rows = relations * rows
    block = (relations + 1) * width // peers
    padded = -(-block // 16) * 16
    bits = peers.bit_length() - 2
    colours = colours_of(bits, padded)
    w_two = jnp.swapaxes(w_two, 1, 2)
    self_two = self_two.T

    near = "V" if table <= 2 * rows else "v"
    vm = pltpu.VMEM
    picks_vm, counts_vm = vm((slots, peers), jnp.int32), vm((1, peers), jnp.int32)
    own_vm, total_vm = vm((rows, width), bf16), vm((8, EXTRA), f32)
    adj_vm, norm_vm = vm((all_rows, table), bf16), vm((all_rows, EXTRA), f32)
    back_vm = vm((table, all_rows), bf16)
    edge_vm = vm((relations, blocks, edges), jnp.int32)
    deep = (relations + 1) * width
    left_vm = vm((rows, deep), bf16)
    turned_vm = vm((deep, rows), bf16 if block % 16 == 0 else f32)
    blocks_vm = vm((2, peers // 2, padded, rows), bf16)
    turn_outs = [((peers // 2, padded, rows), bf16)] * 2
    packed_vm = vm((boundary, width + EXTRA), bf16)

    packed, = call(
        pack_kernel, [((boundary, width + EXTRA), bf16)], (features, picks, send_count, label_row),
        "hhhh", "v", [own_vm, picks_vm, counts_vm, vm((1, rows), jnp.int32)], 4,
        flops=2 * boundary * rows * width, moved=600000,
    )
    got_one = exchange(packed)
    adj, norm, back = call(
        graph_kernel,
        [((all_rows, table), bf16), ((all_rows, EXTRA), f32), ((table, all_rows), bf16)],
        (edge_src, edge_dst), "hh", near + near + "h", [edge_vm] * 2 + [back_vm], 3,
        flops=4 * all_rows * 256 * table, moved=5 << 20,
    )
    left_one, hidden, packed, total = call(
        first_kernel,
        [((rows, deep), bf16), ((rows, width), bf16), ((boundary, width), bf16), ((8, EXTRA), f32)],
        (adj, norm, got_one, features, w_one.reshape(deep, width), picks, send_count),
        near + near + "vhhhh", "hhhh",
        [ own_vm, vm((deep, width), bf16), picks_vm, counts_vm, left_vm,
            own_vm, vm((boundary, width), bf16), total_vm,
        ],
        10,
        flops=2 * all_rows * width * (table + width), moved=10 << 20,
    )
    got_two = exchange(packed)
    keep_one, send_one = call(
        functools.partial(turn_kernel, block), turn_outs, (me, left_one), "sh", "hh",
        [left_vm, turned_vm, blocks_vm], 5, flops=1 << 30, moved=5 << 20,
    )
    other_one = to_pair(send_one)
    logits, keep_two, send_two, grad_logits, local, outgoing = call(
        functools.partial(second_kernel, block),
        [((classes, rows), f32)] + turn_outs
        + [((rows, classes), bf16), ((rows, width), f32), ((boundary, width + EXTRA), bf16)],
        (me, got_two, adj, norm, back, hidden, w_two, self_two, label_row, total), "sv" + near + near + "hhhhhh", "hhhhhh",
        [
            back_vm, own_vm, vm(w_two.shape, bf16),
            vm(self_two.shape, bf16), vm((1, rows), jnp.int32), total_vm, vm((classes, rows), f32),
            turned_vm, blocks_vm, vm((rows, classes), bf16), vm((all_rows, width), bf16),
            vm((rows, width), f32), packed_vm,
        ],
        1 + relations // 2 + 4 + 6,
        flops=8 * all_rows * width * width, moved=16 << 20,
    )
    other_two, other_logits = to_pair(send_two), to_pair(grad_logits)
    returned = exchange(outgoing)
    keep_two, grad_logits = call(
        bring_kernel, [turn_outs[0], ((rows, classes), bf16)], (keep_two, grad_logits), "hh", "VV", (), 2,
        flops=1 << 20, moved=3 << 20, vmem=16,
    )
    parts_two = product(colours, keep_two, other_two, grad_logits, other_logits, "Hv")
    grad_pre, loss = call(
        grad_pre_kernel, [((rows, width), bf16), ((1, 1), f32)],
        (returned, parts_two[0], local, hidden, picks, send_count, total), "vhhhhhh", "Vv",
        [vm((rows, width), f32), own_vm, picks_vm, counts_vm, total_vm], 5,
        flops=2 * rows * boundary * width, moved=2 << 20,
    )
    other_pre = to_pair(grad_pre)
    keep_one, other_one = call(
        bring_kernel, turn_outs, (keep_one, other_one), "hh", "VV", (), 2,
        flops=1 << 20, moved=5 << 20,
    )
    parts_one = product(colours, keep_one, other_one, grad_pre, other_pre, "vv")
    grad_two = scatter_sum(colours, block, parts_two)
    grad_one = scatter_sum(colours, block, parts_one)
    return (logits.T, loss.reshape(()), grad_one, grad_two)


def solution(mesh):
    in_specs = (
        P("dom", None),
        P(),
        P(),
        P(),
        P(None, "dom", None),
        P(None, "dom", None),
        P("dom", None, None),
        P("dom", None),
        P("dom"),
    )
    out_specs = (P("dom", None), P(), P("dom", None), P("dom", None))
    return jax.shard_map(on_device, mesh=mesh, in_specs=in_specs, out_specs=out_specs, check_vma=False)
```

```python
import functools

import jax
import jax.numpy as jnp
from jax import lax
from jax.experimental import pallas as pl
from jax.experimental.pallas import tpu as pltpu
from jax.sharding import PartitionSpec as P


loss_scale = 256.0
bf16 = jnp.bfloat16
f32 = jnp.float32
EXTRA = 128


def dot(a, b):
    return jnp.dot(a, b, preferred_element_type=f32)


def dot_nt(a, b):
    return lax.dot_general(a, b, (((1,), (1,)), ((), ())), preferred_element_type=f32)


def dot_tn(a, b):
    return lax.dot_general(a, b, (((0,), (0,)), ((), ())), preferred_element_type=f32)


def iota(shape, axis):
    return lax.broadcasted_iota(jnp.int32, shape, axis)


def call(body, outs, ins, spaces, out_spaces, scratch=(), copies=0, flops=0, moved=0, vmem=32):
    kinds = {"v": pltpu.VMEM, "V": pltpu.VMEM, "H": pltpu.VMEM, "h": pl.ANY, "s": pltpu.SMEM}
    kept = {"h": pltpu.HBM, "H": pltpu.HBM, "V": pltpu.VMEM}
    scratch = list(scratch)
    if copies:
        scratch.append(pltpu.SemaphoreType.DMA((copies,)))
    ins = [pltpu.with_memory_space_constraint(x, kept[c]) if c in kept else x for x, c in zip(ins, spaces)]
    return pl.pallas_call(
        body,
        out_shape=[kept[c](s, d) if c in kept else jax.ShapeDtypeStruct(s, d) for (s, d), c in zip(outs, out_spaces)],
        in_specs=[pl.BlockSpec(memory_space=kinds[c]) for c in spaces],
        out_specs=[pl.BlockSpec(memory_space=kinds[c]) for c in out_spaces],
        scratch_shapes=scratch,
        compiler_params=pltpu.CompilerParams(vmem_limit_bytes=vmem << 20),
        cost_estimate=pl.CostEstimate(flops=flops, bytes_accessed=moved, transcendentals=0),
    )(*ins)


class Copies:
    def __init__(self, sems):
        self.sems, self.used = sems, 0

    def start(self, source, target):
        copy = pltpu.make_async_copy(source, target, self.sems.at[self.used])
        self.used += 1
        copy.start()
        return copy


def wait_all(copies):
    for copy in copies:
        copy.wait()


def pick_hot(picks, counts, rows):
    slots, peers = picks.shape
    chosen = jnp.where(iota((slots, peers), 0) < counts, picks, -1).astype(f32)
    lane = iota((peers, peers * slots), 1)
    spreader = jnp.where(iota((peers, peers * slots), 0) == lane // slots, 1.0, 0.0)
    if rows <= 256:
        laid = dot(chosen.astype(bf16), spreader.astype(bf16))
    else:
        laid = jnp.dot(chosen, spreader, preferred_element_type=f32, precision=lax.Precision.HIGHEST)
    mine = iota((slots, peers * slots), 0) == iota((slots, peers * slots), 1) % slots
    row = jnp.sum(jnp.where(mine, laid, 0.0), axis=0, keepdims=True)
    hot = iota((rows, peers * slots), 0) == jnp.round(row).astype(jnp.int32)
    return jnp.where(hot, 1.0, 0.0).astype(bf16)


def pack_kernel(feat_hbm, picks_hbm, count_hbm, label_hbm, out_ref, feat, picks, counts, label, sems):
    copies = Copies(sems)
    pairs = ((picks_hbm, picks), (count_hbm, counts), (label_hbm, label), (feat_hbm, feat))
    ins = [copies.start(a, b) for a, b in pairs]
    rows, width = feat.shape
    slots = out_ref.shape[0]
    wait_all(ins[:3])
    hot = pick_hot(picks[...], counts[...], rows)
    count = jnp.sum(jnp.where(label[...] >= 0, 1.0, 0.0), axis=1, keepdims=True)
    high = jnp.floor(count * (1.0 / 128.0))
    low = count - 128.0 * high
    lane = iota((slots, EXTRA), 1)
    out_ref[:, width:] = jnp.where(lane < 64, high, low).astype(bf16)
    ins[3].wait()
    out_ref[:, :width] = dot_tn(hot, feat[...]).astype(bf16)


def graph_kernel(
    src_hbm, dst_hbm, adj_ref, count_ref, back_hbm, src_ref, dst_ref, back_ref, sems
):
    copies = Copies(sems)
    wait_all([copies.start(src_hbm, src_ref), copies.start(dst_hbm, dst_ref)])
    relations, blocks, edges = src_ref.shape
    table = adj_ref.shape[1]

    def step(r, carry):
        for b in range(blocks):
            start = pl.multiple_of((r * blocks + b) * 128, 128)
            src = src_ref[r, b : b + 1, :]
            dst = dst_ref[r, b : b + 1, :]
            hot_dst = jnp.where(iota((128, edges), 0) == dst, 1.0, 0.0)
            hot_src = jnp.where(iota((table, edges), 0) == src, 1.0, 0.0).astype(bf16)
            count = jnp.sum(hot_dst, axis=1, keepdims=True)
            hot_dst = hot_dst.astype(bf16)
            adj_ref[pl.ds(start, 128), :] = dot_nt(hot_dst, hot_src).astype(bf16)
            back_ref[:, pl.ds(start, 128)] = dot_nt(hot_src, hot_dst).astype(bf16)
            count_ref[pl.ds(start, 128), :] = jnp.broadcast_to(count, (128, EXTRA)).astype(bf16)
        return carry

    lax.fori_loop(0, relations, step, 0)
    copies.start(back_ref, back_hbm).wait()


def norm_of(counts, width):
    norm = 1.0 / jnp.maximum(counts.astype(f32), 1.0)
    return jnp.concatenate([norm] * (width // EXTRA), axis=1)


def put_blocks(me, turned, blocks, block):
    pad = blocks.shape[2] - block
    rows = blocks.shape[3]
    for b in range(turned.shape[0] // block):
        place = jnp.bitwise_xor(me, b)
        value = turned[b * block : (b + 1) * block, :].astype(bf16)
        if pad:
            value = jnp.concatenate([value, jnp.zeros((pad, rows), bf16)], axis=0)
        blocks[jnp.bitwise_and(place, 1), jnp.right_shift(place, 1)] = value


def first_kernel(
    adj, norm, got_ref, feat_hbm, w_hbm, picks_hbm, count_hbm,
    left_hbm, hid, hid_hbm, pack_hbm, total_hbm,
    feat, w, picks, counts, left, packed, total_ref, sems,
):
    copies = Copies(sems)
    rows, width = feat.shape
    relations = w.shape[0] // width - 1
    chunks = [slice(r * rows, (r + 2) * rows) for r in range(0, relations, 2)]
    near = [copies.start(feat_hbm, feat)]
    w_in = []
    parts = [slice(0, 4 * width), slice(4 * width, 7 * width), slice(7 * width, (relations + 1) * width)]
    for at in parts:
        w_in.append(copies.start(w_hbm.at[at, :], w.at[at, :]))
    small = [copies.start(picks_hbm, picks), copies.start(count_hbm, counts)]
    wait_all(near)
    own = feat[...]
    got = got_ref[:, :width]
    left[:, relations * width :] = own
    for i, at in enumerate(chunks):
        sums = dot(adj[at, :rows], own) + dot(adj[at, rows:], got)
        avg = (sums * norm_of(norm[at, :], width)).astype(bf16)
        left[:, 2 * i * width : (2 * i + 1) * width] = avg[:rows]
        left[:, (2 * i + 1) * width : (2 * i + 2) * width] = avg[rows:]
    out = [copies.start(left, left_hbm)]
    wait_all(small)
    hot = pick_hot(picks[...], counts[...], rows)
    total = None
    for i, at in enumerate(parts):
        w_in[i].wait()
        part = dot(left[:, at], w[at, :])
        total = part if total is None else total + part
    hidden = jnp.maximum(total, 0.0).astype(bf16)
    packed[...] = dot_tn(hot, hidden).astype(bf16)
    out.append(copies.start(packed, pack_hbm))
    hid[...] = hidden
    out.append(copies.start(hid, hid_hbm))
    sums = jnp.sum(got_ref[:, width:].astype(f32), axis=0, keepdims=True)
    count = (sums[:, 0:1] * 128.0 + sums[:, 64:65]) * 0.125
    total_ref[...] = jnp.broadcast_to(count, total_ref.shape)
    out.append(copies.start(total_ref, total_hbm))
    wait_all(out)


def second_kernel(
    block, me_ref, got_ref, adj, norm, hid, back_hbm, w_hbm, self_hbm, label_hbm, total_hbm,
    logit_hbm, keep_hbm, send_hbm, grad_hbm, spread_hbm, out_hbm,
    back, w, selfs, label, total, logit, turned, blocks, grad_ref, spreads,
    packed, sems,
):
    copies = Copies(sems)
    rows, width = hid.shape
    relations, classes, _ = w.shape
    chunks = [slice(r * rows, (r + 2) * rows) for r in range(0, relations, 2)]
    w_in = []
    for i in range(len(chunks)):
        w_in.append(copies.start(w_hbm.at[2 * i : 2 * i + 2], w.at[2 * i : 2 * i + 2]))
    small = [copies.start(a, b) for a, b in ((self_hbm, selfs), (label_hbm, label), (total_hbm, total))]
    back_in = copies.start(back_hbm.at[rows:, :], back)
    own = hid[...]
    got = got_ref[...]
    logits = None
    turned[relations * width :, :] = own.T.astype(turned.dtype)
    for i, at in enumerate(chunks):
        sums = dot(adj[at, :rows], own) + dot(adj[at, rows:], got)
        avg = (sums * norm_of(norm[at, :], width)).astype(bf16)
        w_in[i].wait()
        part = dot_nt(w[2 * i], avg[:rows]) + dot_nt(w[2 * i + 1], avg[rows:])
        logits = part if logits is None else logits + part
        for j in range(2):
            where = slice((2 * i + j) * width, (2 * i + j + 1) * width)
            turned[where, :] = avg[j * rows : (j + 1) * rows].T.astype(turned.dtype)
    wait_all(small)
    logits = logits + dot_nt(selfs[...], own)
    logit[...] = logits
    out = [copies.start(logit, logit_hbm)]
    put_blocks(me_ref[0], turned, blocks, block)
    out += [copies.start(blocks.at[0], keep_hbm), copies.start(blocks.at[1], send_hbm)]
    count = total[0:1, 0:1]
    labels = label[...]
    labelled = jnp.where(labels >= 0, 1.0, 0.0)
    hot = jnp.where(iota((classes, rows), 0) == labels, 1.0, 0.0)
    peak = jnp.max(logits, axis=0, keepdims=True)
    log_total = peak + jnp.log(jnp.sum(jnp.exp(logits - peak), axis=0, keepdims=True))
    picked = jnp.sum(logits * hot, axis=0, keepdims=True)
    local = jnp.sum(jnp.where(labels >= 0, log_total - picked, 0.0), axis=1, keepdims=True)
    soft = jnp.exp(logits - log_total)
    grad = (loss_scale * (soft - hot) * labelled / count).T.astype(bf16)
    grad_ref[...] = grad
    out.append(copies.start(grad_ref, grad_hbm))
    for r in range(relations):
        at = slice(r * rows, (r + 1) * rows)
        spread = dot(grad, w[r]) * norm_of(norm[at, :], width)
        spreads[at, :] = spread.astype(bf16)
        if r % 4 == 3:
            part = slice((r - 3) * rows, (r + 1) * rows)
            out.append(copies.start(spreads.at[part, :], spread_hbm.at[part, :]))
    slots = packed.shape[0]
    first = local.astype(bf16).astype(f32)
    second = (local - first).astype(bf16).astype(f32)
    third = local - first - second
    lane = iota((slots, EXTRA), 1)
    packed[:, width:] = jnp.where(lane < 32, first, jnp.where(lane < 64, second, third)).astype(bf16)
    back_in.wait()
    packed[:, :width] = dot(back[...], spreads[...]).astype(bf16)
    out.append(copies.start(packed, out_hbm))
    wait_all(out)


def turn_kernel(block, me_ref, left_hbm, keep_hbm, send_hbm, left, turned, blocks, sems):
    copies = Copies(sems)
    step = turned.shape[0] // 3
    cuts = [slice(i * step, (i + 1) * step) for i in range(3)]
    ins = [copies.start(left_hbm.at[:, at], left.at[:, at]) for at in cuts]
    for at, copy in zip(cuts, ins):
        copy.wait()
        turned[at, :] = left[:, at].T.astype(turned.dtype)
    put_blocks(me_ref[0], turned, blocks, block)
    wait_all([copies.start(blocks.at[0], keep_hbm), copies.start(blocks.at[1], send_hbm)])


def grad_pre_kernel(
    got_ref, after_ref, local_hbm, hid_hbm, picks_hbm, count_hbm, total_hbm,
    out_ref, loss_ref, local, hid, picks, counts, total, sems,
):
    copies = Copies(sems)
    pairs = (
        (picks_hbm, picks), (count_hbm, counts), (local_hbm, local), (hid_hbm, hid), (total_hbm, total),
    )
    ins = [copies.start(a, b) for a, b in pairs]
    wait_all(ins[:2])
    rows, width = local.shape
    grad = dot(pick_hot(picks[...], counts[...], rows), got_ref[:, :width])
    sums = jnp.sum(got_ref[:, width:].astype(f32), axis=0, keepdims=True)
    loss = (sums[:, 0:1] + sums[:, 32:33] + sums[:, 64:65]) * 0.125
    wait_all(ins[2:])
    out_ref[...] = jnp.where(hid[...].astype(f32) > 0.0, local[...] + grad, 0.0).astype(bf16)
    loss_ref[...] = loss / total[0:1, 0:1]


def local_kernel(
    keep_hbm, grad_hbm, back_hbm, spread_hbm, self_hbm, keep_ref, grad_ref, local_hbm,
    back, spreads, selfs, local, sems,
):
    copies = Copies(sems)
    rows = local.shape[0]
    first = copies.start(grad_hbm, grad_ref), copies.start(self_hbm, selfs)
    brought = copies.start(keep_hbm, keep_ref)
    ins = copies.start(back_hbm.at[:rows, :], back), copies.start(spread_hbm, spreads)
    wait_all(first)
    own = dot(grad_ref[...], selfs[...])
    wait_all(ins)
    local[...] = dot(back[...], spreads[...]) + own
    copies.start(local, local_hbm).wait()
    brought.wait()


def bring_kernel(*refs):
    count = len(refs) // 2
    copies = Copies(refs[-1])
    wait_all([copies.start(a, b) for a, b in zip(refs[:count], refs[count : 2 * count])])


class Colour:
    def __init__(self, start, size, order):
        self.start, self.size, self.order = start, size, order

    def places(self, stage):
        gone = self.order[:stage]
        bits = len(self.order)
        return [p for p in range(1 << bits) if not any(p >> g & 1 for g in gone)]

    def split(self, stage):
        bit = self.order[stage]
        here = self.places(stage)
        return [p for p in here if p >> bit & 1], [p for p in here if not p >> bit & 1]


ORDERS_ONE = [[0, 1, 3, 2], [1, 2, 0, 3], [2, 0, 1, 3]]
ORDERS_TWO = [[0, 1, 3, 2], [2, 0, 1, 3], [2, 0, 1, 3]]


def colours_of(bits, rows, orders):
    tiles = rows // 16
    last = list(range(4, bits))
    third = tiles // 3
    sizes = [tiles - 2 * third, third, third]
    out, at = [], 0
    for size, order in zip(sizes, orders):
        if size:
            out.append(Colour(at * 16, size * 16, order + last))
        at += size
    return out


def product_kernel(colours, keep_ref, other_ref, grad_ref, other_grad_ref, *outs):
    grad, other_grad = grad_ref[...], other_grad_ref[...]
    width = grad.shape[1]
    for i, colour in enumerate(colours):
        rows = slice(colour.start, colour.start + colour.size)
        for places, out in zip(colour.split(0), outs[2 * i : 2 * i + 2]):
            left = jnp.concatenate([keep_ref[p, rows, :] for p in places], axis=0)
            right = jnp.concatenate([other_ref[p, rows, :] for p in places], axis=0)
            value = dot(left, grad) + dot(right, other_grad)
            out[...] = value.astype(out.dtype).reshape(len(places), colour.size, width)


def add_kernel(colour, stage, got, kept, *outs):
    here = colour.places(stage)
    for places, out in zip(colour.split(stage), outs):
        for j, p in enumerate(places):
            k = here.index(p)
            out[j] = (kept[k] + got[k].astype(f32)).astype(out.dtype)


def join_kernel(colours, stage, *refs):
    count = len(colours)
    ins, (sent, stay) = refs[: 2 * count], refs[2 * count :]
    at = 0
    for i, colour in enumerate(colours):
        got, kept = ins[2 * i], ins[2 * i + 1]
        here = colour.places(stage)
        for places, out in zip(colour.split(stage), (sent, stay)):
            k = here.index(places[0])
            value = (kept[k] + got[k].astype(f32)).astype(out.dtype)
            out[at : at + colour.size, :] = value
        at += colour.size


def last_kernel(groups, block, *refs):
    out = refs[-1]
    for i, group in enumerate(groups):
        value = refs[2 * i + 1][...] + refs[2 * i][...].astype(f32)
        at = 0
        for colour in group:
            size = min(colour.size, block - colour.start)
            if size > 0:
                out[colour.start : colour.start + size, :] = value[at : at + size]
            at += colour.size


def across(value, bit):
    size = lax.axis_size("dom")
    return lax.ppermute(value, "dom", [(i, i ^ (2 << bit)) for i in range(size)])


def to_pair(value):
    size = lax.axis_size("dom")
    return lax.ppermute(value, "dom", [(i, i ^ 1) for i in range(size)])


def product(colours, keep, other, grad, other_grad, spaces):
    width = grad.shape[1]
    outs = []
    for colour in colours:
        sent, kept = colour.split(0)
        outs.append(((len(sent), colour.size, width), bf16))
        outs.append(((len(kept), colour.size, width), f32))
    ins = (keep, other, grad, other_grad)
    return call(
        functools.partial(product_kernel, colours), outs, ins, "vvvv", spaces * len(colours),
        flops=4 * keep.size * width, moved=keep.size * 12, vmem=16,
    )


def add_stage(colour, stage, got, kept):
    sent, keep = colour.split(stage)
    outs = [((len(sent),) + got.shape[1:], bf16), ((len(keep),) + got.shape[1:], f32)]
    return call(
        functools.partial(add_kernel, colour, stage), outs, (got, kept), "vv", "vv",
        flops=got.size * 200, moved=got.size * 10, vmem=4,
    )


def groups_of(colours):
    last = {}
    for i, colour in enumerate(colours):
        last.setdefault(colour.order[-1], []).append(i)
    return list(last.values())


def scatter_sum(colours, block, parts):
    bits = len(colours[0].order)
    states = [list(parts[2 * i : 2 * i + 2]) for i in range(len(colours))]
    for stage in range(bits - 1):
        for i, colour in enumerate(colours):
            sent, kept = states[i]
            got = across(sent, colour.order[stage])
            if stage + 2 < bits:
                states[i] = add_stage(colour, stage + 1, got, kept)
            else:
                states[i] = [got, kept]
    ends, groups = [], []
    for group in groups_of(colours):
        members = [colours[i] for i in group]
        ins = [x for i in group for x in states[i]]
        shape = (sum(c.size for c in members), ins[0].shape[2])
        sent, kept = call(
            functools.partial(join_kernel, members, bits - 1), [(shape, bf16), (shape, f32)], ins,
            "v" * len(ins), "vv", flops=shape[0] * 1000, moved=shape[0] * 9000, vmem=4,
        )
        ends += [across(sent, members[0].order[-1]), kept]
        groups.append(members)
    return call(
        functools.partial(last_kernel, groups, block), [((block, ends[0].shape[1]), f32)], ends,
        "v" * len(ends), "v", flops=block * 1000, moved=block * 5000, vmem=4,
    )[0]


def exchange(value):
    peers = lax.axis_size("dom")
    slots = value.shape[0] // peers
    cut = value.reshape(peers, slots, value.shape[1])
    got = lax.all_to_all(cut, "dom", split_axis=0, concat_axis=0, tiled=True)
    return got.reshape(value.shape)


def on_device(features, w_one, w_two, self_two, edge_src, edge_dst, send_rows, send_count, labels):
    peers = lax.axis_size("dom")
    rows, width = features.shape
    relations, _, classes = w_two.shape
    blocks, edges = edge_src.shape[1:]
    picks = send_rows[0].T
    slots = picks.shape[0]
    boundary = peers * slots
    table = rows + boundary
    label_row = labels.reshape(1, rows)
    me = lax.axis_index("dom").astype(jnp.int32).reshape(1)
    all_rows = relations * rows
    block = (relations + 1) * width // peers
    padded = -(-block // 16) * 16
    bits = peers.bit_length() - 2
    shares_one = colours_of(bits, padded, ORDERS_ONE)
    shares_two = colours_of(bits, padded, ORDERS_TWO)
    w_two = jnp.swapaxes(w_two, 1, 2)
    self_two = self_two.T

    near = "V" if table <= 2 * rows else "v"
    vm = pltpu.VMEM
    picks_vm, counts_vm = vm((slots, peers), jnp.int32), vm((1, peers), jnp.int32)
    own_vm, total_vm = vm((rows, width), bf16), vm((8, EXTRA), f32)
    adj_vm, norm_vm = vm((all_rows, table), bf16), vm((all_rows, EXTRA), f32)
    back_vm = vm((table, all_rows), bf16)
    edge_vm = vm((relations, blocks, edges), jnp.int32)
    deep = (relations + 1) * width
    left_vm = vm((rows, deep), bf16)
    turned_vm = vm((deep, rows), bf16 if block % 16 == 0 else f32)
    blocks_vm = vm((2, peers // 2, padded, rows), bf16)
    turn_outs = [((peers // 2, padded, rows), bf16)] * 2
    packed_vm = vm((boundary, width + EXTRA), bf16)

    packed, = call(
        pack_kernel, [((boundary, width + EXTRA), bf16)], (features, picks, send_count, label_row),
        "hhhh", "v", [own_vm, picks_vm, counts_vm, vm((1, rows), jnp.int32)], 4,
        flops=2 * boundary * rows * width, moved=600000,
    )
    got_one = exchange(packed)
    adj, norm, back = call(
        graph_kernel,
        [((all_rows, table), bf16), ((all_rows, EXTRA), bf16), ((table, all_rows), bf16)],
        (edge_src, edge_dst), "hh", near + near + "h", [edge_vm] * 2 + [back_vm], 3,
        flops=4 * all_rows * 256 * table, moved=5 << 20,
    )
    left_one, hidden_near, hidden, packed, total = call(
        first_kernel,
        [((rows, deep), bf16)] + [((rows, width), bf16)] * 2
        + [((boundary, width), bf16), ((8, EXTRA), f32)],
        (adj, norm, got_one, features, w_one.reshape(deep, width), picks, send_count),
        near + near + "vhhhh", "h" + near + "hhh",
        [
            own_vm, vm((deep, width), bf16), picks_vm, counts_vm, left_vm, vm((boundary, width), bf16), total_vm,
        ],
        10,
        flops=2 * all_rows * width * (table + width), moved=10 << 20,
    )
    got_two = exchange(packed)
    keep_one, send_one = call(
        functools.partial(turn_kernel, block), turn_outs, (me, left_one), "sh", "hh",
        [left_vm, turned_vm, blocks_vm], 5, flops=1 << 30, moved=5 << 20,
    )
    other_one = to_pair(send_one)
    logits, keep_two, send_two, grad_logits, spread, outgoing = call(
        functools.partial(second_kernel, block),
        [((classes, rows), f32)] + turn_outs
        + [((rows, classes), bf16), ((all_rows, width), bf16), ((boundary, width + EXTRA), bf16)],
        (me, got_two, adj, norm, hidden_near, back, w_two, self_two, label_row, total),
        "sv" + near * 3 + "hhhhh", "hhhhhh",
        [
            vm((boundary, all_rows), bf16), vm(w_two.shape, bf16),
            vm(self_two.shape, bf16), vm((1, rows), jnp.int32), total_vm, vm((classes, rows), f32),
            turned_vm, blocks_vm, vm((rows, classes), bf16), vm((all_rows, width), bf16),
            packed_vm,
        ],
        relations // 2 + 4 + 5 + relations // 4,
        flops=8 * all_rows * width * width, moved=16 << 20,
    )
    other_two, other_logits = to_pair(send_two), to_pair(grad_logits)
    returned = exchange(outgoing)
    keep_two, grad_logits, local = call(
        local_kernel, [turn_outs[0], ((rows, classes), bf16), ((rows, width), f32)],
        (keep_two, grad_logits, back, spread, self_two), "hhhhh", "VVh",
        [
            vm((rows, all_rows), bf16), vm((all_rows, width), bf16), vm(self_two.shape, bf16),
            vm((rows, width), f32),
        ], 6,
        flops=1 << 20, moved=3 << 20,
    )
    parts_two = product(shares_two, keep_two, other_two, grad_logits, other_logits, "Hv")
    grad_pre, loss = call(
        grad_pre_kernel, [((rows, width), bf16), ((1, 1), f32)],
        (returned, parts_two[0], local, hidden, picks, send_count, total), "vhhhhhh", "Vv",
        [vm((rows, width), f32), own_vm, picks_vm, counts_vm, total_vm], 5,
        flops=2 * rows * boundary * width, moved=2 << 20,
    )
    other_pre = to_pair(grad_pre)
    keep_one, other_one = call(
        bring_kernel, turn_outs, (keep_one, other_one), "hh", "VV", (), 2,
        flops=1 << 20, moved=5 << 20,
    )
    parts_one = product(shares_one, keep_one, other_one, grad_pre, other_pre, "vv")
    grad_two = scatter_sum(shares_two, block, parts_two)
    grad_one = scatter_sum(shares_one, block, parts_one)
    return (logits.T, loss.reshape(()), grad_one, grad_two)


def solution(mesh):
    in_specs = (
        P("dom", None),
        P(),
        P(),
        P(),
        P(None, "dom", None),
        P(None, "dom", None),
        P("dom", None, None),
        P("dom", None),
        P("dom"),
    )
    out_specs = (P("dom", None), P(), P("dom", None), P("dom", None))
    return jax.shard_map(on_device, mesh=mesh, in_specs=in_specs, out_specs=out_specs, check_vma=False)
```

```python
import functools

import jax
import jax.numpy as jnp
from jax import lax
from jax.experimental import pallas as pl
from jax.experimental.pallas import tpu as pltpu
from jax.sharding import PartitionSpec as P


loss_scale = 256.0
bf16 = jnp.bfloat16
f32 = jnp.float32
HEAD = 16
EXTRA = 128


def dot(a, b):
    return jnp.dot(a, b, preferred_element_type=f32)


def dot_nt(a, b):
    return lax.dot_general(a, b, (((1,), (1,)), ((), ())), preferred_element_type=f32)


def dot_tn(a, b):
    return lax.dot_general(a, b, (((0,), (0,)), ((), ())), preferred_element_type=f32)


def iota(shape, axis):
    return lax.broadcasted_iota(jnp.int32, shape, axis)


def call(body, outs, ins, spaces, out_spaces, scratch=(), copies=0, flops=0, moved=0, vmem=32):
    kinds = {"v": pltpu.VMEM, "V": pltpu.VMEM, "H": pltpu.VMEM, "h": pl.ANY, "s": pltpu.SMEM}
    kept = {"h": pltpu.HBM, "H": pltpu.HBM, "V": pltpu.VMEM}
    scratch = list(scratch)
    if copies:
        scratch.append(pltpu.SemaphoreType.DMA((copies,)))
    ins = [pltpu.with_memory_space_constraint(x, kept[c]) if c in kept else x for x, c in zip(ins, spaces)]
    return pl.pallas_call(
        body,
        out_shape=[kept[c](s, d) if c in kept else jax.ShapeDtypeStruct(s, d) for (s, d), c in zip(outs, out_spaces)],
        in_specs=[pl.BlockSpec(memory_space=kinds[c]) for c in spaces],
        out_specs=[pl.BlockSpec(memory_space=kinds[c]) for c in out_spaces],
        scratch_shapes=scratch,
        compiler_params=pltpu.CompilerParams(vmem_limit_bytes=vmem << 20),
        cost_estimate=pl.CostEstimate(flops=flops, bytes_accessed=moved, transcendentals=0),
    )(*ins)


class Copies:
    def __init__(self, sems):
        self.sems, self.used = sems, 0

    def start(self, source, target):
        copy = pltpu.make_async_copy(source, target, self.sems.at[self.used])
        self.used += 1
        copy.start()
        return copy


def wait_all(copies):
    for copy in copies:
        copy.wait()


def pick_hot(picks, counts, rows):
    slots, peers = picks.shape
    chosen = jnp.where(iota((slots, peers), 0) < counts, picks, -1).astype(f32)
    lane = iota((peers, peers * slots), 1)
    spreader = jnp.where(iota((peers, peers * slots), 0) == lane // slots, 1.0, 0.0)
    if rows <= 256:
        laid = dot(chosen.astype(bf16), spreader.astype(bf16))
    else:
        laid = jnp.dot(chosen, spreader, preferred_element_type=f32, precision=lax.Precision.HIGHEST)
    mine = iota((slots, peers * slots), 0) == iota((slots, peers * slots), 1) % slots
    row = jnp.sum(jnp.where(mine, laid, 0.0), axis=0, keepdims=True)
    hot = iota((rows, peers * slots), 0) == jnp.round(row).astype(jnp.int32)
    return jnp.where(hot, 1.0, 0.0).astype(bf16)


def pack_kernel(feat_hbm, picks_hbm, count_hbm, label_hbm, out_ref, feat, picks, counts, label, sems):
    copies = Copies(sems)
    pairs = ((picks_hbm, picks), (count_hbm, counts), (label_hbm, label), (feat_hbm, feat))
    ins = [copies.start(a, b) for a, b in pairs]
    rows, width = feat.shape
    slots = out_ref.shape[0]
    wait_all(ins[:3])
    hot = pick_hot(picks[...], counts[...], rows)
    count = jnp.sum(jnp.where(label[...] >= 0, 1.0, 0.0), axis=1, keepdims=True)
    high = jnp.floor(count * (1.0 / 128.0))
    low = count - 128.0 * high
    lane = iota((slots, EXTRA), 1)
    out_ref[:, width:] = jnp.where(lane < 64, high, low).astype(bf16)
    ins[3].wait()
    out_ref[:, :width] = dot_tn(hot, feat[...]).astype(bf16)


def graph_kernel(
    src_hbm, dst_hbm, adj_ref, count_ref, back_hbm, src_ref, dst_ref, back_ref, sems
):
    copies = Copies(sems)
    wait_all([copies.start(src_hbm, src_ref), copies.start(dst_hbm, dst_ref)])
    relations, blocks, edges = src_ref.shape
    table = adj_ref.shape[1]

    def step(r, carry):
        for b in range(blocks):
            start = pl.multiple_of((r * blocks + b) * 128, 128)
            src = src_ref[r, b : b + 1, :]
            dst = dst_ref[r, b : b + 1, :]
            hot_dst = jnp.where(iota((128, edges), 0) == dst, 1.0, 0.0)
            hot_src = jnp.where(iota((table, edges), 0) == src, 1.0, 0.0).astype(bf16)
            count = jnp.sum(hot_dst, axis=1, keepdims=True)
            hot_dst = hot_dst.astype(bf16)
            adj_ref[pl.ds(start, 128), :] = dot_nt(hot_dst, hot_src).astype(bf16)
            back_ref[:, pl.ds(start, 128)] = dot_nt(hot_src, hot_dst).astype(bf16)
            count_ref[pl.ds(start, 128), :] = jnp.broadcast_to(count, (128, EXTRA)).astype(bf16)
        return carry

    lax.fori_loop(0, relations, step, 0)
    copies.start(back_ref, back_hbm).wait()


def norm_of(counts, width):
    norm = 1.0 / jnp.maximum(counts.astype(f32), 1.0)
    return jnp.concatenate([norm] * (width // EXTRA), axis=1)


def pieces(value, place):
    first = value.astype(bf16).astype(f32)
    second = (value - first).astype(bf16).astype(f32)
    return jnp.where(place == 0, first, jnp.where(place == 1, second, value - first - second))


def add_up(value, classes):
    return value[:, classes : classes + 1] + value[:, classes + 1 : classes + 2] + value[:, classes + 2 : classes + 3]


def put_total(value, total, classes, dtype):
    lane = iota(value.shape, 1)
    if dtype == bf16:
        behind = pieces(total, lane - classes)
    else:
        behind = jnp.where(lane == classes, total, 0.0)
    return jnp.where(lane < classes, value, behind).astype(dtype)


def put_blocks(me, turned, blocks, block):
    pad = blocks.shape[2] - block
    rows = blocks.shape[3]
    for b in range(turned.shape[0] // block):
        place = jnp.bitwise_xor(me, b)
        value = turned[b * block : (b + 1) * block, :].astype(bf16)
        if pad:
            value = jnp.concatenate([value, jnp.zeros((pad, rows), bf16)], axis=0)
        blocks[jnp.bitwise_and(place, 1), jnp.right_shift(place, 1)] = value


def first_kernel(
    adj, norm, got_ref, feat_hbm, w_hbm, picks_hbm, count_hbm,
    left_hbm, hid, hid_hbm, pack_hbm, total_hbm,
    feat, w, picks, counts, left, packed, total_ref, sems,
):
    copies = Copies(sems)
    rows, width = feat.shape
    relations = w.shape[0] // width - 1
    chunks = [slice(r * rows, (r + 2) * rows) for r in range(0, relations, 2)]
    near = [copies.start(feat_hbm, feat)]
    w_in = []
    parts = [slice(0, 4 * width), slice(4 * width, 7 * width), slice(7 * width, (relations + 1) * width)]
    for at in parts:
        w_in.append(copies.start(w_hbm.at[at, :], w.at[at, :]))
    small = [copies.start(picks_hbm, picks), copies.start(count_hbm, counts)]
    wait_all(near)
    own = feat[...]
    got = got_ref[:, :width]
    left[:, relations * width :] = own
    for i, at in enumerate(chunks):
        sums = dot(adj[at, :rows], own) + dot(adj[at, rows:], got)
        avg = (sums * norm_of(norm[at, :], width)).astype(bf16)
        left[:, 2 * i * width : (2 * i + 1) * width] = avg[:rows]
        left[:, (2 * i + 1) * width : (2 * i + 2) * width] = avg[rows:]
    out = [copies.start(left, left_hbm)]
    wait_all(small)
    hot = pick_hot(picks[...], counts[...], rows)
    total = None
    for i, at in enumerate(parts):
        w_in[i].wait()
        part = dot(left[:, at], w[at, :])
        total = part if total is None else total + part
    hidden = jnp.maximum(total, 0.0).astype(bf16)
    packed[...] = dot_tn(hot, hidden).astype(bf16)
    out.append(copies.start(packed, pack_hbm))
    hid[...] = hidden
    out.append(copies.start(hid, hid_hbm))
    sums = jnp.sum(got_ref[:, width:].astype(f32), axis=0, keepdims=True)
    count = (sums[:, 0:1] * 128.0 + sums[:, 64:65]) * 0.125
    total_ref[...] = jnp.broadcast_to(count, total_ref.shape)
    out.append(copies.start(total_ref, total_hbm))
    wait_all(out)


def second_kernel(
    block, me_ref, got_ref, adj, norm, hid, back_hbm, w_hbm, self_hbm, label_hbm, total_hbm,
    logit_hbm, keep_hbm, send_hbm, grad_hbm, spread_hbm, out_hbm,
    back, w, selfs, label, total, logit, turned, blocks, grad_ref, spreads,
    packed, sems,
):
    copies = Copies(sems)
    rows, width = hid.shape
    relations, classes, _ = w.shape
    chunks = [slice(r * rows, (r + 2) * rows) for r in range(0, relations, 2)]
    w_in = []
    for i in range(len(chunks)):
        w_in.append(copies.start(w_hbm.at[2 * i : 2 * i + 2], w.at[2 * i : 2 * i + 2]))
    small = [copies.start(a, b) for a, b in ((self_hbm, selfs), (label_hbm, label), (total_hbm, total))]
    back_in = copies.start(back_hbm.at[rows:, :], back)
    own = hid[...]
    got = got_ref[...]
    logits = None
    turned[relations * width :, :] = own.T.astype(turned.dtype)
    for i, at in enumerate(chunks):
        sums = dot(adj[at, :rows], own) + dot(adj[at, rows:], got)
        avg = (sums * norm_of(norm[at, :], width)).astype(bf16)
        w_in[i].wait()
        part = dot_nt(w[2 * i], avg[:rows]) + dot_nt(w[2 * i + 1], avg[rows:])
        logits = part if logits is None else logits + part
        for j in range(2):
            where = slice((2 * i + j) * width, (2 * i + j + 1) * width)
            turned[where, :] = avg[j * rows : (j + 1) * rows].T.astype(turned.dtype)
    wait_all(small)
    logits = logits + dot_nt(selfs[...], own)
    logit[...] = logits
    out = [copies.start(logit, logit_hbm)]
    put_blocks(me_ref[0], turned, blocks, block)
    out += [copies.start(blocks.at[0], keep_hbm), copies.start(blocks.at[1], send_hbm)]
    count = total[0:1, 0:1]
    labels = label[...]
    labelled = jnp.where(labels >= 0, 1.0, 0.0)
    hot = jnp.where(iota((classes, rows), 0) == labels, 1.0, 0.0)
    peak = jnp.max(logits, axis=0, keepdims=True)
    log_total = peak + jnp.log(jnp.sum(jnp.exp(logits - peak), axis=0, keepdims=True))
    picked = jnp.sum(logits * hot, axis=0, keepdims=True)
    local = jnp.sum(jnp.where(labels >= 0, log_total - picked, 0.0), axis=1, keepdims=True)
    soft = jnp.exp(logits - log_total)
    grad = (loss_scale * (soft - hot) * labelled / count).T.astype(bf16)
    grad_ref[:, :classes] = grad
    grad_ref[:, classes:] = pieces(jnp.broadcast_to(local, (rows, 1)), iota((rows, 3), 1)).astype(bf16)
    out.append(copies.start(grad_ref, grad_hbm))
    for r in range(relations):
        at = slice(r * rows, (r + 1) * rows)
        spread = dot(grad, w[r]) * norm_of(norm[at, :], width)
        spreads[at, :] = spread.astype(bf16)
        if r % 4 == 3:
            part = slice((r - 3) * rows, (r + 1) * rows)
            out.append(copies.start(spreads.at[part, :], spread_hbm.at[part, :]))
    back_in.wait()
    packed[...] = dot(back[...], spreads[...]).astype(bf16)
    out.append(copies.start(packed, out_hbm))
    wait_all(out)


def turn_kernel(block, me_ref, left_hbm, keep_hbm, send_hbm, left, turned, blocks, sems):
    copies = Copies(sems)
    step = turned.shape[0] // 3
    cuts = [slice(i * step, (i + 1) * step) for i in range(3)]
    ins = [copies.start(left_hbm.at[:, at], left.at[:, at]) for at in cuts]
    for at, copy in zip(cuts, ins):
        copy.wait()
        turned[at, :] = left[:, at].T.astype(turned.dtype)
    put_blocks(me_ref[0], turned, blocks, block)
    wait_all([copies.start(blocks.at[0], keep_hbm), copies.start(blocks.at[1], send_hbm)])


def grad_pre_kernel(
    got_ref, after_ref, local_hbm, hid_hbm, picks_hbm, count_hbm, out_ref, local, hid, picks, counts, sems
):
    copies = Copies(sems)
    pairs = ((picks_hbm, picks), (count_hbm, counts), (local_hbm, local), (hid_hbm, hid))
    ins = [copies.start(a, b) for a, b in pairs]
    wait_all(ins[:2])
    grad = dot(pick_hot(picks[...], counts[...], local.shape[0]), got_ref[...])
    wait_all(ins[2:])
    out_ref[...] = jnp.where(hid[...].astype(f32) > 0.0, local[...] + grad, 0.0).astype(bf16)


def local_kernel(
    keep_hbm, grad_hbm, back_hbm, spread_hbm, self_hbm, keep_ref, grad_ref, local_hbm,
    back, spreads, selfs, local, sems,
):
    copies = Copies(sems)
    rows = local.shape[0]
    first = copies.start(grad_hbm, grad_ref), copies.start(self_hbm, selfs)
    brought = copies.start(keep_hbm, keep_ref)
    ins = copies.start(back_hbm.at[:rows, :], back), copies.start(spread_hbm, spreads)
    wait_all(first)
    own = dot(grad_ref[:, : selfs.shape[0]], selfs[...])
    wait_all(ins)
    local[...] = dot(back[...], spreads[...]) + own
    copies.start(local, local_hbm).wait()
    brought.wait()


def bring_kernel(*refs):
    count = len(refs) // 2
    copies = Copies(refs[-1])
    wait_all([copies.start(a, b) for a, b in zip(refs[:count], refs[count : 2 * count])])


class Colour:
    def __init__(self, start, size, order):
        self.start, self.size, self.order = start, size, order

    def places(self, stage):
        gone = self.order[:stage]
        bits = len(self.order)
        return [p for p in range(1 << bits) if not any(p >> g & 1 for g in gone)]

    def split(self, stage):
        bit = self.order[stage]
        here = self.places(stage)
        return [p for p in here if p >> bit & 1], [p for p in here if not p >> bit & 1]


ORDERS_ONE = [[0, 1, 3, 2], [2, 0, 1, 3], [1, 2, 0, 3]]
ORDERS_TWO = [[2, 0, 1, 3], [1, 2, 0, 3]]


def colours_of(bits, rows, orders):
    tiles = rows // 16
    last = list(range(4, bits))
    share = tiles // len(orders)
    sizes = [tiles - share * (len(orders) - 1)] + [share] * (len(orders) - 1)
    out, at = [], 0
    for size, order in zip(sizes, orders):
        if size:
            out.append(Colour(at * 16, size * 16, order + last))
        at += size
    return out


def product_kernel(colours, classes, keep_ref, other_ref, grad_ref, other_grad_ref, *outs):
    grad, other_grad = grad_ref[...], other_grad_ref[...]
    width = grad.shape[1]
    if classes:
        total = add_up(grad[:1].astype(f32), classes) + add_up(other_grad[:1].astype(f32), classes)
    for i, colour in enumerate(colours):
        rows = slice(colour.start, colour.start + colour.size)
        for places, out in zip(colour.split(0), outs[2 * i : 2 * i + 2]):
            left = jnp.concatenate([keep_ref[p, rows, :] for p in places], axis=0)
            right = jnp.concatenate([other_ref[p, rows, :] for p in places], axis=0)
            value = dot(left, grad) + dot(right, other_grad)
            out[...] = value.astype(out.dtype).reshape(len(places), colour.size, width)
            if classes and i == 0:
                for j in range(len(places)):
                    head = value[j * colour.size : j * colour.size + HEAD]
                    out[j, :HEAD, :] = put_total(head, total, classes, out.dtype)


def add_kernel(colour, stage, classes, got, kept, *outs):
    here = colour.places(stage)
    for places, out in zip(colour.split(stage), outs):
        for j, p in enumerate(places):
            k = here.index(p)
            value = kept[k] + got[k].astype(f32)
            out[j] = value.astype(out.dtype)
            if classes:
                head = value[:HEAD]
                out[j, :HEAD, :] = put_total(head, add_up(head, classes), classes, out.dtype)


def join_kernel(colours, stage, classes, *refs):
    count = len(colours)
    ins, (sent, stay) = refs[: 2 * count], refs[2 * count :]
    at = 0
    for i, colour in enumerate(colours):
        got, kept = ins[2 * i], ins[2 * i + 1]
        here = colour.places(stage)
        for places, out in zip(colour.split(stage), (sent, stay)):
            k = here.index(places[0])
            value = kept[k] + got[k].astype(f32)
            out[at : at + colour.size, :] = value.astype(out.dtype)
            if classes and i == 0:
                head = value[:HEAD]
                out[:HEAD, :] = put_total(head, add_up(head, classes), classes, out.dtype)
        at += colour.size


def last_kernel(groups, block, classes, *refs):
    out = refs[2 * len(groups) + (1 if classes else 0)]
    if classes:
        value = refs[1][:HEAD, :] + refs[0][:HEAD, :].astype(f32)
        refs[-1][...] = add_up(value, classes)[:1] / refs[2 * len(groups)][0:1, 0:1]
    for i, group in enumerate(groups):
        value = refs[2 * i + 1][...] + refs[2 * i][...].astype(f32)
        at = 0
        for colour in group:
            size = min(colour.size, block - colour.start)
            if size > 0:
                out[colour.start : colour.start + size, :] = value[at : at + size, : out.shape[1]]
            at += colour.size


def across(value, bit):
    size = lax.axis_size("dom")
    return lax.ppermute(value, "dom", [(i, i ^ (2 << bit)) for i in range(size)])


def to_pair(value):
    size = lax.axis_size("dom")
    return lax.ppermute(value, "dom", [(i, i ^ 1) for i in range(size)])


def product(colours, classes, keep, other, grad, other_grad, spaces):
    width = grad.shape[1]
    outs = []
    for colour in colours:
        sent, kept = colour.split(0)
        outs.append(((len(sent), colour.size, width), bf16))
        outs.append(((len(kept), colour.size, width), f32))
    ins = (keep, other, grad, other_grad)
    return call(
        functools.partial(product_kernel, colours, classes), outs, ins, "vvvv", spaces * len(colours),
        flops=4 * keep.size * width, moved=keep.size * 12, vmem=16,
    )


def add_stage(colour, stage, classes, got, kept):
    sent, keep = colour.split(stage)
    outs = [((len(sent),) + got.shape[1:], bf16), ((len(keep),) + got.shape[1:], f32)]
    return call(
        functools.partial(add_kernel, colour, stage, classes), outs, (got, kept), "vv", "vv",
        flops=got.size * 200, moved=got.size * 10, vmem=4,
    )


def groups_of(colours):
    last = {}
    for i, colour in enumerate(colours):
        last.setdefault(colour.order[-1], []).append(i)
    return list(last.values())


def scatter_sum(colours, block, parts, classes=0, count=None):
    bits = len(colours[0].order)
    states = [list(parts[2 * i : 2 * i + 2]) for i in range(len(colours))]
    for stage in range(bits - 1):
        for i, colour in enumerate(colours):
            sent, kept = states[i]
            got = across(sent, colour.order[stage])
            if stage + 2 < bits:
                states[i] = add_stage(colour, stage + 1, 0 if i else classes, got, kept)
            else:
                states[i] = [got, kept]
    ends, groups = [], []
    for j, group in enumerate(groups_of(colours)):
        members = [colours[i] for i in group]
        ins = [x for i in group for x in states[i]]
        shape = (sum(c.size for c in members), ins[0].shape[2])
        sent, kept = call(
            functools.partial(join_kernel, members, bits - 1, 0 if j else classes), [(shape, bf16), (shape, f32)], ins,
            "v" * len(ins), "vv", flops=shape[0] * 1000, moved=shape[0] * 9000, vmem=4,
        )
        ends += [across(sent, members[0].order[-1]), kept]
        groups.append(members)
    outs = [((block, classes or ends[0].shape[1]), f32)]
    if classes:
        ends.append(count)
        outs.append(((1, 1), f32))
    return call(
        functools.partial(last_kernel, groups, block, classes), outs, ends,
        "v" * len(ends), "v" * len(outs), flops=block * 1000, moved=block * 5000, vmem=4,
    )


def exchange(value):
    peers = lax.axis_size("dom")
    slots = value.shape[0] // peers
    cut = value.reshape(peers, slots, value.shape[1])
    got = lax.all_to_all(cut, "dom", split_axis=0, concat_axis=0, tiled=True)
    return got.reshape(value.shape)


def on_device(features, w_one, w_two, self_two, edge_src, edge_dst, send_rows, send_count, labels):
    peers = lax.axis_size("dom")
    rows, width = features.shape
    relations, _, classes = w_two.shape
    blocks, edges = edge_src.shape[1:]
    picks = send_rows[0].T
    slots = picks.shape[0]
    boundary = peers * slots
    table = rows + boundary
    label_row = labels.reshape(1, rows)
    me = lax.axis_index("dom").astype(jnp.int32).reshape(1)
    all_rows = relations * rows
    block = (relations + 1) * width // peers
    padded = -(-block // 16) * 16
    bits = peers.bit_length() - 2
    shares_one = colours_of(bits, padded, ORDERS_ONE)
    shares_two = colours_of(bits, padded, ORDERS_TWO)
    w_two = jnp.swapaxes(w_two, 1, 2)
    self_two = self_two.T

    near = "V" if table <= 2 * rows else "v"
    vm = pltpu.VMEM
    picks_vm, counts_vm = vm((slots, peers), jnp.int32), vm((1, peers), jnp.int32)
    own_vm, total_vm = vm((rows, width), bf16), vm((8, EXTRA), f32)
    adj_vm, norm_vm = vm((all_rows, table), bf16), vm((all_rows, EXTRA), f32)
    back_vm = vm((table, all_rows), bf16)
    edge_vm = vm((relations, blocks, edges), jnp.int32)
    deep = (relations + 1) * width
    left_vm = vm((rows, deep), bf16)
    turned_vm = vm((deep, rows), bf16 if block % 16 == 0 else f32)
    blocks_vm = vm((2, peers // 2, padded, rows), bf16)
    turn_outs = [((peers // 2, padded, rows), bf16)] * 2
    packed_vm = vm((boundary, width + EXTRA), bf16)

    packed, = call(
        pack_kernel, [((boundary, width + EXTRA), bf16)], (features, picks, send_count, label_row),
        "hhhh", "v", [own_vm, picks_vm, counts_vm, vm((1, rows), jnp.int32)], 4,
        flops=2 * boundary * rows * width, moved=600000,
    )
    got_one = exchange(packed)
    adj, norm, back = call(
        graph_kernel,
        [((all_rows, table), bf16), ((all_rows, EXTRA), bf16), ((table, all_rows), bf16)],
        (edge_src, edge_dst), "hh", near + near + "h", [edge_vm] * 2 + [back_vm], 3,
        flops=4 * all_rows * 256 * table, moved=5 << 20,
    )
    left_one, hidden_near, hidden, packed, total = call(
        first_kernel,
        [((rows, deep), bf16)] + [((rows, width), bf16)] * 2
        + [((boundary, width), bf16), ((8, EXTRA), f32)],
        (adj, norm, got_one, features, w_one.reshape(deep, width), picks, send_count),
        near + near + "vhhhh", "h" + near + "hhh",
        [
            own_vm, vm((deep, width), bf16), picks_vm, counts_vm, left_vm, vm((boundary, width), bf16), total_vm,
        ],
        10,
        flops=2 * all_rows * width * (table + width), moved=10 << 20,
    )
    got_two = exchange(packed)
    keep_one, send_one = call(
        functools.partial(turn_kernel, block), turn_outs, (me, left_one), "sh", "hh",
        [left_vm, turned_vm, blocks_vm], 5, flops=1 << 30, moved=5 << 20,
    )
    other_one = to_pair(send_one)
    logits, keep_two, send_two, grad_logits, spread, outgoing = call(
        functools.partial(second_kernel, block),
        [((classes, rows), f32)] + turn_outs
        + [((rows, classes + 3), bf16), ((all_rows, width), bf16), ((boundary, width), bf16)],
        (me, got_two, adj, norm, hidden_near, back, w_two, self_two, label_row, total),
        "sv" + near * 3 + "hhhhh", "hhhhhh",
        [
            vm((boundary, all_rows), bf16), vm(w_two.shape, bf16),
            vm(self_two.shape, bf16), vm((1, rows), jnp.int32), total_vm, vm((classes, rows), f32),
            turned_vm, blocks_vm, vm((rows, classes + 3), bf16), vm((all_rows, width), bf16),
            vm((boundary, width), bf16),
        ],
        relations // 2 + 4 + 5 + relations // 4,
        flops=8 * all_rows * width * width, moved=16 << 20,
    )
    other_two, other_logits = to_pair(send_two), to_pair(grad_logits)
    returned = exchange(outgoing)
    keep_two, grad_logits, local = call(
        local_kernel, [turn_outs[0], ((rows, classes + 3), bf16), ((rows, width), f32)],
        (keep_two, grad_logits, back, spread, self_two), "hhhhh", "VVh",
        [
            vm((rows, all_rows), bf16), vm((all_rows, width), bf16), vm(self_two.shape, bf16),
            vm((rows, width), f32),
        ], 6,
        flops=1 << 20, moved=3 << 20,
    )
    parts_two = product(shares_two, classes, keep_two, other_two, grad_logits, other_logits, "Hv")
    grad_pre, = call(
        grad_pre_kernel, [((rows, width), bf16)],
        (returned, parts_two[0], local, hidden, picks, send_count), "vhhhhh", "V",
        [vm((rows, width), f32), own_vm, picks_vm, counts_vm], 4,
        flops=2 * rows * boundary * width, moved=2 << 20,
    )
    other_pre = to_pair(grad_pre)
    keep_one, other_one = call(
        bring_kernel, turn_outs, (keep_one, other_one), "hh", "VV", (), 2,
        flops=1 << 20, moved=5 << 20,
    )
    parts_one = product(shares_one, 0, keep_one, other_one, grad_pre, other_pre, "vv")
    grad_two, loss = scatter_sum(shares_two, block, parts_two, classes, total)
    grad_one, = scatter_sum(shares_one, block, parts_one)
    return (logits.T, loss.reshape(()), grad_one, grad_two)


def solution(mesh):
    in_specs = (
        P("dom", None),
        P(),
        P(),
        P(),
        P(None, "dom", None),
        P(None, "dom", None),
        P("dom", None, None),
        P("dom", None),
        P("dom"),
    )
    out_specs = (P("dom", None), P(), P("dom", None), P("dom", None))
    return jax.shard_map(on_device, mesh=mesh, in_specs=in_specs, out_specs=out_specs, check_vma=False)
```
